256 devices in a mesh: tr: 4 (over x), tc: 4 (over y_hi, core), st: 16 (over y_lo, z).
Axes of the slice: x: 4, y: 4 (y_hi: 2, y_lo: 2; y = y_hi * 2 + y_lo), z: 8, core: 2. Of those that a mesh axis runs over, the one named last changes fastest.
Arguments:
- teacher_hidden: bfloat16 [256, 28672], P(None, 'st'), may hold values from -6 to 6
- teacher_residual: bfloat16 [256, 8192], P(None, ('tr', 'tc')), may hold values from -6 to 6
- teacher_down: bfloat16 [28672, 8192], P('st', ('tr', 'tc')), may hold values from -0.03125 to 0.03125
- student_input: bfloat16 [256, 4096], P(None, 'st'), may hold values from -6 to 6
- student_stream: bfloat16 [256, 4096], P(None, 'st'), may hold values from -6 to 6
- student_gate: bfloat16 [4096, 14336], P('st', ('tr', 'tc')), may hold values from -0.09375 to 0.09375
- student_up: bfloat16 [4096, 14336], P('st', ('tr', 'tc')), may hold values from -0.09375 to 0.09375
- student_down: bfloat16 [14336, 4096], P(('tr', 'tc'), 'st'), may hold values from -0.046875 to 0.046875
- head: bfloat16 [4096, 8192], P('st', ('tr', 'tc')), may hold values from -0.09375 to 0.09375
Outputs:
- grad_gate: float32 [4096, 14336], P('st', ('tr', 'tc'))
- grad_up: float32 [4096, 14336], P('st', ('tr', 'tc'))
- grad_down: float32 [14336, 4096], P(('tr', 'tc'), 'st')
- grad_head: float32 [4096, 8192], P('st', ('tr', 'tc'))
The draws below stay inside these ranges and needn't reach their ends.
All inputs are finite; a program needn't handle non-finite values.
Results may differ from the reference program's by a relative error of at most 0.0065.
Values may be sent and summed in bfloat16 or wider, within the bound.
A program may use at most 64 MiB of HBM per device.

```python
import math
import jax
import jax.numpy as jnp
from jax import lax

DT = 8192
FT = 28672
DS = 4096
FS = 14336
TOKENS = 256


def block_levels(key, shape, cuts, low, high):
    def one(axis_at, blocks):
        steps = jax.random.uniform(jax.random.fold_in(jax.random.fold_in(key, 6), axis_at), (blocks,), jnp.float32, low / len(cuts), high / len(cuts))
        return jnp.repeat(jnp.exp(steps), shape[axis_at] // blocks).reshape((-1,) + (1,) * (len(shape) - axis_at - 1))

    factor_of = one(*cuts[0])
    for cut in cuts[1:]:
        factor_of = factor_of * one(*cut)
    return factor_of


def gaussian(own_key, shape, width, reach, split=(), dtype=jnp.bfloat16):
    drawn = jax.random.normal(own_key, shape, jnp.float32) * width
    if len(split) > 0:
        drawn = block_levels(own_key, shape, split, -0.22, 0.18) * drawn
    return jnp.clip(drawn, min=-reach, max=reach).astype(dtype)


def setup_inputs(seed: int = 0) -> dict:
    keys = jax.random.split(jax.random.key(seed), 10)
    teacher_hidden = gaussian(keys[0], (TOKENS, FT), 1.0, 6.0, ((1, 16),))
    teacher_residual = gaussian(keys[1], (TOKENS, DT), 1.0, 6.0, ((1, 16),))
    teacher_down = gaussian(keys[2], (FT, DT), FT ** -0.5, 0.03125, ((0, 16), (1, 16)))
    student_input = gaussian(keys[3], (TOKENS, DS), 1.0, 6.0, ((1, 16),))
    student_stream = gaussian(keys[4], (TOKENS, DS), 1.0, 6.0, ((1, 16),))
    student_gate = gaussian(keys[5], (DS, FS), DS ** -0.5, 0.09375, ((0, 16), (1, 16)))
    student_up = gaussian(keys[6], (DS, FS), DS ** -0.5, 0.09375, ((0, 16), (1, 16)))
    student_down = gaussian(keys[7], (FS, DS), FS ** -0.5, 0.046875, ((0, 16), (1, 16)))
    head = gaussian(keys[8], (DS, DT), DS ** -0.5, 0.09375, ((0, 16), (1, 16)))
    return {"teacher_hidden": teacher_hidden, "teacher_residual": teacher_residual, "teacher_down": teacher_down, "student_input": student_input, "student_stream": student_stream, "student_gate": student_gate, "student_up": student_up, "student_down": student_down, "head": head}


def contract_rows(left, right):
    return lax.dot_general(left, right, (((0,), (0,)), ((), ())), preferred_element_type=jnp.float32)

def contract_cols(left, right):
    return lax.dot_general(left, right, (((1,), (1,)), ((), ())), preferred_element_type=jnp.float32)

def activation_grads(hidden_grad, gate, up):
    sigma = jax.nn.sigmoid(gate)
    gated = gate * sigma
    slope = sigma * (1.0 + gate * (1.0 - sigma))
    return ((hidden_grad * up * slope).astype(jnp.bfloat16), (hidden_grad * gated).astype(jnp.bfloat16))

def reference(teacher_hidden, teacher_residual, teacher_down, student_input, student_stream, student_gate, student_up, student_down, head):
    loss_scale = 1.0 / math.sqrt(TOKENS)
    teacher_output = teacher_residual.astype(jnp.float32) + jnp.dot(teacher_hidden, teacher_down, preferred_element_type=jnp.float32)
    gate = jnp.dot(student_input, student_gate, preferred_element_type=jnp.float32)
    up = jnp.dot(student_input, student_up, preferred_element_type=jnp.float32)
    hidden = (jax.nn.silu(gate) * up).astype(jnp.bfloat16)
    features = (student_stream.astype(jnp.float32) + jnp.dot(hidden, student_down, preferred_element_type=jnp.float32)).astype(jnp.bfloat16)
    error = jnp.dot(features, head, preferred_element_type=jnp.float32) - teacher_output
    signal = (error * loss_scale).astype(jnp.bfloat16)
    grad_head = contract_rows(features, signal)
    feature_grad = contract_cols(signal, head).astype(jnp.bfloat16)
    grad_down = contract_rows(hidden, feature_grad)
    hidden_grad = contract_cols(feature_grad, student_down)
    gate_signal, up_signal = activation_grads(hidden_grad, gate, up)
    grad_gate = contract_rows(student_input, gate_signal)
    grad_up = contract_rows(student_input, up_signal)
    return (grad_gate, grad_up, grad_down, grad_head)
```

```python
import functools
import math

import jax
import jax.numpy as jnp
from jax import lax
from jax.experimental import pallas as pl
from jax.experimental.pallas import tpu as pltpu
from jax.sharding import PartitionSpec as P

BF = jnp.bfloat16
F32 = jnp.float32
MESH = pl.DeviceIdType.MESH
N = 16
OTHERS = N - 1


def dot(a, b):
    return jnp.dot(a, b, preferred_element_type=F32)


def dot_cols(a, b):
    return lax.dot_general(a, b, (((1,), (1,)), ((), ())), preferred_element_type=F32)


def contract_rows(left, right):
    return lax.dot_general(
        left, right, (((0,), (0,)), ((), ())), preferred_element_type=F32
    )


def kernel(
    tc_size,
    th, res, td, xin, stream, wg, wu, wd, hd,
    o_hid, o_feat, o_sig, o_fg, o_gs, o_us,
    v_th, v_res, v_td, v_x, v_stream, v_wg, v_wu, v_wd, v_hd,
    f1, p1, r1, g2s, g2, f3, p3, r3, g3s, g3, f4, p4, r4, g5s, g5,
    f6, p6, r6, g6s, g6, f7, p7, r7, g8as, g8a, g8bs, g8b,
    gate_ref, up_ref,
    load_sem, out_sem, send_sem, recv_sem,
):
    tokens = p1.shape[0]
    rows = tokens // N
    fs = wg.shape[1]
    st = lax.axis_index("st")
    grp = lax.axis_index("tr") * tc_size + lax.axis_index("tc")

    def st_peer(k):
        p = lax.rem(st + k, N)
        return p, {"st": p}

    def grp_peer(k):
        p = lax.rem(grp + k, N)
        return p, {"tr": p // tc_size, "tc": lax.rem(p, tc_size)}

    def at_rows(ref, i):
        return ref.at[pl.ds(pl.multiple_of(i * rows, rows), rows), :]

    loads = [
        pltpu.make_async_copy(src, dst, load_sem.at[i])
        for i, (src, dst) in enumerate(
            [
                (xin, v_x), (wg, v_wg), (wu, v_wu), (th, v_th), (td, v_td),
                (wd, v_wd), (hd, v_hd), (at_rows(stream, grp), v_stream),
                (at_rows(res, st), v_res),
            ]
        )
    ]
    for c in loads:
        c.start()

    barrier = pltpu.get_barrier_semaphore()

    def greet(k, carry):
        for peer in (st_peer, grp_peer):
            pl.semaphore_signal(barrier, inc=1, device_id=peer(k)[1], device_id_type=MESH)
        return carry

    lax.fori_loop(1, N, greet, 0)

    def scatter(i, peer, part, slots):
        def one(k, carry):
            p, device = peer(k)
            pltpu.make_async_remote_copy(
                src_ref=at_rows(part, p), dst_ref=slots.at[OTHERS - k],
                send_sem=send_sem.at[i], recv_sem=recv_sem.at[i],
                device_id=device, device_id_type=MESH,
            ).start()
            return carry

        lax.fori_loop(1, N, one, 0)

    def arrived(i, slots):
        pltpu.make_async_copy(slots, slots, recv_sem.at[i]).wait()

    def summed(i, own, slots):
        arrived(i, slots)
        total = own
        for k in range(OTHERS):
            total = total + slots[k].astype(F32)
        return total

    def spread(i, peer, share, whole, me):
        def one(k, carry):
            device = peer(k)[1]
            pltpu.make_async_remote_copy(
                src_ref=share, dst_ref=at_rows(whole, me),
                send_sem=send_sem.at[i], recv_sem=recv_sem.at[i],
                device_id=device, device_id_type=MESH,
            ).start()
            return carry

        lax.fori_loop(1, N, one, 0)

    def gathered(i, whole):
        most = whole.at[pl.ds(0, OTHERS * rows), :]
        pltpu.make_async_copy(most, most, recv_sem.at[i]).wait()

    def sent(i, like):
        most = like.at[pl.ds(0, OTHERS * rows), :]
        pltpu.make_async_copy(most, most, send_sem.at[i]).wait()

    def put(ref, i, value):
        ref[pl.ds(pl.multiple_of(i * rows, rows), rows), :] = value

    def get(ref, i):
        return ref[pl.ds(pl.multiple_of(i * rows, rows), rows), :]

    outs = []

    def out(src, dst):
        c = pltpu.make_async_copy(src, dst, out_sem.at[len(outs)])
        c.start()
        outs.append(c)

    for c in loads[:3]:
        c.wait()
    for w, at in ((v_wg, 0), (v_wu, fs)):
        part = dot(v_x[...], w[...])
        f1[:, pl.ds(at, fs)] = part
        p1[:, pl.ds(at, fs)] = part.astype(BF)
    pl.semaphore_wait(barrier, 2 * OTHERS)
    scatter(0, st_peer, p1, r1)
    for c in loads[3:]:
        c.wait()
    f4[...] = dot(v_th[...], v_td[...])
    both = summed(0, get(f1, st), r1)
    gate, up = both[:, :fs], both[:, fs:]
    gate_ref[...] = gate
    up_ref[...] = up
    share = (gate * jax.nn.sigmoid(gate) * up).astype(BF)
    g2s[...] = share
    spread(1, st_peer, g2s, g2, st)
    put(g2, st, share)
    gathered(1, g2)
    part = dot(g2[...], v_wd[...])
    f3[...] = part
    p3[...] = part.astype(BF)
    scatter(2, grp_peer, p3, r3)
    out(g2, o_hid)
    total = summed(2, get(f3, grp), r3)
    share = (v_stream[...].astype(F32) + total).astype(BF)
    g3s[...] = share
    spread(3, grp_peer, g3s, g3, grp)
    put(g3, grp, share)
    gathered(3, g3)
    part = dot(g3[...], v_hd[...]) - f4[...]
    f4[...] = part
    p4[...] = part.astype(BF)
    scatter(4, st_peer, p4, r4)
    out(g3, o_feat)
    total = summed(4, get(f4, st), r4)
    share = ((total - v_res[...].astype(F32)) * (1.0 / math.sqrt(tokens))).astype(BF)
    g5s[...] = share
    spread(5, st_peer, g5s, g5, st)
    put(g5, st, share)
    gathered(5, g5)
    part = dot_cols(g5[...], v_hd[...])
    f6[...] = part
    p6[...] = part.astype(BF)
    scatter(6, grp_peer, p6, r6)
    out(g5, o_sig)
    share = summed(6, get(f6, grp), r6).astype(BF)
    g6s[...] = share
    spread(7, grp_peer, g6s, g6, grp)
    put(g6, grp, share)
    gathered(7, g6)
    part = dot_cols(g6[...], v_wd[...])
    f7[...] = part
    p7[...] = part.astype(BF)
    scatter(8, st_peer, p7, r7)
    out(g6, o_fg)
    gate, up = gate_ref[...], up_ref[...]
    sigma = jax.nn.sigmoid(gate)
    grad = summed(8, get(f7, st), r7)
    gate_share = (grad * up * (sigma * (1.0 + gate * (1.0 - sigma)))).astype(BF)
    up_share = (grad * (gate * sigma)).astype(BF)
    g8as[...] = gate_share
    spread(9, st_peer, g8as, g8a, st)
    g8bs[...] = up_share
    spread(10, st_peer, g8bs, g8b, st)
    put(g8a, st, gate_share)
    put(g8b, st, up_share)
    gathered(9, g8a)
    out(g8a, o_gs)
    gathered(10, g8b)
    out(g8b, o_us)
    for i, like in enumerate((p1, g2, p3, g3, p4, g5, p6, g6, p7, g8a, g8b)):
        sent(i, like)
    for c in outs:
        c.wait()


def body(
    teacher_hidden, teacher_residual, teacher_down, student_input, student_stream,
    student_gate, student_up, student_down, head,
):
    tokens, ds = student_input.shape
    fs = student_gate.shape[1]
    dt = head.shape[1]
    rows = tokens // N
    arguments = (
        teacher_hidden, teacher_residual, teacher_down, student_input, student_stream,
        student_gate, student_up, student_down, head,
    )
    vm = lambda shape, dtype: pltpu.VMEM(shape, dtype)

    def reduce_bufs(cols):
        return [vm((tokens, cols), F32), vm((tokens, cols), BF), vm((OTHERS, rows, cols), BF)]

    def gather_bufs(cols):
        return [vm((rows, cols), BF), vm((tokens, cols), BF)]

    staged = [
        vm((rows, a.shape[1]), a.dtype) if i in (1, 4) else vm(a.shape, a.dtype)
        for i, a in enumerate(arguments)
    ]
    scratch = (
        staged
        + reduce_bufs(2 * fs) + gather_bufs(fs)
        + reduce_bufs(ds) + gather_bufs(ds)
        + reduce_bufs(dt) + gather_bufs(dt)
        + reduce_bufs(ds) + gather_bufs(ds)
        + reduce_bufs(fs) + gather_bufs(fs) + gather_bufs(fs)
        + [vm((rows, fs), F32), vm((rows, fs), F32)]
        + [
            pltpu.SemaphoreType.DMA((9,)),
            pltpu.SemaphoreType.DMA((6,)),
            pltpu.SemaphoreType.DMA((11,)),
            pltpu.SemaphoreType.DMA((11,)),
        ]
    )
    shapes = [(tokens, c) for c in (fs, ds, dt, ds, fs, fs)]
    hidden, features, signal, feature_grad, gate_signal, up_signal = pl.pallas_call(
        functools.partial(kernel, lax.axis_size("tc")),
        out_shape=[jax.ShapeDtypeStruct(s, BF) for s in shapes],
        in_specs=[pl.BlockSpec(memory_space=pl.ANY)] * 9,
        out_specs=[pl.BlockSpec(memory_space=pl.ANY)] * 6,
        scratch_shapes=scratch,
        compiler_params=pltpu.CompilerParams(
            collective_id=0, has_side_effects=True, vmem_limit_bytes=56 << 20
        ),
        name="chain",
    )(*arguments)
    return (
        contract_rows(student_input, gate_signal),
        contract_rows(student_input, up_signal),
        contract_rows(hidden, feature_grad),
        contract_rows(features, signal),
    )


def solution(mesh):
    in_specs = (
        P(None, "st"),
        P(None, ("tr", "tc")),
        P("st", ("tr", "tc")),
        P(None, "st"),
        P(None, "st"),
        P("st", ("tr", "tc")),
        P("st", ("tr", "tc")),
        P(("tr", "tc"), "st"),
        P("st", ("tr", "tc")),
    )
    out_specs = (
        P("st", ("tr", "tc")),
        P("st", ("tr", "tc")),
        P(("tr", "tc"), "st"),
        P("st", ("tr", "tc")),
    )
    return jax.shard_map(body, mesh=mesh, in_specs=in_specs, out_specs=out_specs, check_vma=False)
```

```python
import functools
import math

import jax
import jax.numpy as jnp
from jax import lax
from jax.experimental import pallas as pl
from jax.experimental.pallas import tpu as pltpu
from jax.sharding import PartitionSpec as P

BF = jnp.bfloat16
F32 = jnp.float32
MESH = pl.DeviceIdType.MESH
N = 16
OTHERS = N - 1


def dot(a, b):
    return jnp.dot(a, b, preferred_element_type=F32)


def dot_cols(a, b):
    return lax.dot_general(a, b, (((1,), (1,)), ((), ())), preferred_element_type=F32)


def contract_rows(left, right):
    return lax.dot_general(
        left, right, (((0,), (0,)), ((), ())), preferred_element_type=F32
    )


def kernel(
    tc_size,
    th, res, td, xin, stream, wg, wu, wd, hd,
    o_hid, o_feat, o_sig, o_fg, o_gs, o_us,
    v_th, v_res, v_td, v_x, v_stream, v_wg, v_wu, v_wd, v_hd,
    f1, p1, r1, g2s, g2, f3, p3, r3, g3s, g3, f4, p4, r4, g5s, g5,
    f6, p6, r6, g6s, g6, f7, p7, r7, g8s, g8,
    gates, gate_ref, ups, up_ref, by_gate, by_up, s_gate, s_up,
    load_sem, out_sem, send_sem, recv_sem,
):
    tokens = p1.shape[0]
    rows = tokens // N
    fs = wg.shape[1]
    st = lax.axis_index("st")
    grp = lax.axis_index("tr") * tc_size + lax.axis_index("tc")

    def st_peer(k):
        p = lax.rem(st + k, N)
        return p, {"st": p}

    def grp_peer(k):
        p = lax.rem(grp + k, N)
        return p, {"tr": p // tc_size, "tc": lax.rem(p, tc_size)}

    def at_rows(ref, i):
        return ref.at[pl.ds(pl.multiple_of(i * rows, rows), rows), :]

    loads = [
        pltpu.make_async_copy(src, dst, load_sem.at[i])
        for i, (src, dst) in enumerate(
            [
                (xin, v_x), (wg, v_wg), (wu, v_wu), (th, v_th), (td, v_td),
                (wd, v_wd), (hd, v_hd), (at_rows(stream, grp), v_stream),
                (at_rows(res, st), v_res),
            ]
        )
    ]
    for c in loads:
        c.start()

    barrier = pltpu.get_barrier_semaphore()

    def greet(k, carry):
        for peer in (st_peer, grp_peer):
            pl.semaphore_signal(barrier, inc=1, device_id=peer(k)[1], device_id_type=MESH)
        return carry

    lax.fori_loop(1, N, greet, 0)

    def scatter(i, peer, part, slots):
        def one(k, carry):
            p, device = peer(k)
            pltpu.make_async_remote_copy(
                src_ref=at_rows(part, p), dst_ref=slots.at[OTHERS - k],
                send_sem=send_sem.at[i], recv_sem=recv_sem.at[i],
                device_id=device, device_id_type=MESH,
            ).start()
            return carry

        lax.fori_loop(1, N, one, 0)

    def arrived(i, slots):
        pltpu.make_async_copy(slots, slots, recv_sem.at[i]).wait()

    def summed(i, own, slots):
        arrived(i, slots)
        total = own
        for k in range(OTHERS):
            total = total + slots[k].astype(F32)
        return total

    def spread(i, peer, share, whole, me):
        def one(k, carry):
            device = peer(k)[1]
            pltpu.make_async_remote_copy(
                src_ref=share, dst_ref=at_rows(whole, me),
                send_sem=send_sem.at[i], recv_sem=recv_sem.at[i],
                device_id=device, device_id_type=MESH,
            ).start()
            return carry

        lax.fori_loop(1, N, one, 0)

    def gathered(i, whole):
        most = whole.at[pl.ds(0, OTHERS * rows), :]
        pltpu.make_async_copy(most, most, recv_sem.at[i]).wait()

    def sent(i, like):
        most = like.at[pl.ds(0, OTHERS * rows), :]
        pltpu.make_async_copy(most, most, send_sem.at[i]).wait()

    def put(ref, i, value):
        ref[pl.ds(pl.multiple_of(i * rows, rows), rows), :] = value

    def get(ref, i):
        return ref[pl.ds(pl.multiple_of(i * rows, rows), rows), :]

    outs = []

    def out(src, dst):
        c = pltpu.make_async_copy(src, dst, out_sem.at[len(outs)])
        c.start()
        outs.append(c)

    for c in loads[:3]:
        c.wait()
    for w, at in ((v_wg, 0), (v_wu, fs)):
        part = dot(v_x[...], w[...])
        f1[:, pl.ds(at, fs)] = part
        p1[:, pl.ds(at, fs)] = part.astype(BF)
    pl.semaphore_wait(barrier, 2 * OTHERS)
    scatter(0, st_peer, p1, r1)
    for c in loads[3:]:
        c.wait()
    f4[...] = dot(v_th[...], v_td[...])
    both = summed(0, get(f1, st), r1)
    gate, up = both[:, :fs], both[:, fs:]
    gates[...] = gate.astype(BF)
    ups[...] = up.astype(BF)
    share = (gate * jax.nn.sigmoid(gate) * up).astype(BF)
    g2s[...] = share
    spread(1, st_peer, g2s, g2, st)
    put(g2, st, share)
    put(gate_ref, st, gates[...])
    put(up_ref, st, ups[...])
    gathered(1, g2)
    part = dot(g2[...], v_wd[...])
    f3[...] = part
    p3[...] = part.astype(BF)
    scatter(2, grp_peer, p3, r3)
    spread(9, st_peer, gates, gate_ref, st)
    out(g2, o_hid)
    total = summed(2, get(f3, grp), r3)
    share = (v_stream[...].astype(F32) + total).astype(BF)
    g3s[...] = share
    spread(3, grp_peer, g3s, g3, grp)
    put(g3, grp, share)
    gathered(3, g3)
    part = dot(g3[...], v_hd[...]) - f4[...]
    f4[...] = part
    p4[...] = part.astype(BF)
    scatter(4, st_peer, p4, r4)
    out(g3, o_feat)
    total = summed(4, get(f4, st), r4)
    share = ((total - v_res[...].astype(F32)) * (1.0 / math.sqrt(tokens))).astype(BF)
    g5s[...] = share
    spread(5, st_peer, g5s, g5, st)
    put(g5, st, share)
    gathered(5, g5)
    part = dot_cols(g5[...], v_hd[...])
    f6[...] = part
    p6[...] = part.astype(BF)
    scatter(6, grp_peer, p6, r6)
    spread(10, st_peer, ups, up_ref, st)
    out(g5, o_sig)
    share = summed(6, get(f6, grp), r6).astype(BF)
    g6s[...] = share
    spread(7, grp_peer, g6s, g6, grp)
    put(g6, grp, share)
    gathered(7, g6)
    part = dot_cols(g6[...], v_wd[...])
    f7[...] = part
    p7[...] = part.astype(BF)
    scatter(8, st_peer, p7, r7)
    out(g6, o_fg)
    gathered(9, gate_ref)
    gathered(10, up_ref)
    gate = gate_ref[...].astype(F32)
    sigma = jax.nn.sigmoid(gate)
    by_gate[...] = up_ref[...].astype(F32) * (sigma * (1.0 + gate * (1.0 - sigma)))
    by_up[...] = gate * sigma
    share = summed(8, get(f7, st), r7).astype(BF)
    g8s[...] = share
    spread(11, st_peer, g8s, g8, st)
    put(g8, st, share)
    gathered(11, g8)
    grad = g8[...].astype(F32)
    s_gate[...] = (grad * by_gate[...]).astype(BF)
    out(s_gate, o_gs)
    s_up[...] = (grad * by_up[...]).astype(BF)
    out(s_up, o_us)
    for i, like in enumerate((p1, g2, p3, g3, p4, g5, p6, g6, p7, gate_ref, up_ref, g8)):
        sent(i, like)
    for c in outs:
        c.wait()


def gradients(
    x, gs, us, hid, fg, feat, sig, o_gate, o_up, o_down, o_head,
    v_x, v_gs, v_us, v_hid, v_fg, v_feat, v_sig, r_gate, r_up, r_down, r_head,
    load_sem, out_sem,
):
    pairs = [
        (feat, v_feat), (sig, v_sig), (hid, v_hid), (fg, v_fg),
        (x, v_x), (gs, v_gs), (us, v_us),
    ]
    loads = [
        pltpu.make_async_copy(src, dst, load_sem.at[i]) for i, (src, dst) in enumerate(pairs)
    ]
    for c in loads:
        c.start()
    stores = []
    for need, left, right, result, dest in (
        (2, v_feat, v_sig, r_head, o_head),
        (2, v_hid, v_fg, r_down, o_down),
        (2, v_x, v_gs, r_gate, o_gate),
        (1, v_x, v_us, r_up, o_up),
    ):
        for c in loads[:need]:
            c.wait()
        loads = loads[need:]
        result[...] = contract_rows(left[...], right[...])
        c = pltpu.make_async_copy(result, dest, out_sem.at[len(stores)])
        c.start()
        stores.append(c)
    for c in stores:
        c.wait()


def body(
    teacher_hidden, teacher_residual, teacher_down, student_input, student_stream,
    student_gate, student_up, student_down, head,
):
    tokens, ds = student_input.shape
    fs = student_gate.shape[1]
    dt = head.shape[1]
    rows = tokens // N
    arguments = (
        teacher_hidden, teacher_residual, teacher_down, student_input, student_stream,
        student_gate, student_up, student_down, head,
    )
    vm = lambda shape, dtype: pltpu.VMEM(shape, dtype)

    def reduce_bufs(cols):
        return [vm((tokens, cols), F32), vm((tokens, cols), BF), vm((OTHERS, rows, cols), BF)]

    def gather_bufs(cols):
        return [vm((rows, cols), BF), vm((tokens, cols), BF)]

    staged = [
        vm((rows, a.shape[1]), a.dtype) if i in (1, 4) else vm(a.shape, a.dtype)
        for i, a in enumerate(arguments)
    ]
    scratch = (
        staged
        + reduce_bufs(2 * fs) + gather_bufs(fs)
        + reduce_bufs(ds) + gather_bufs(ds)
        + reduce_bufs(dt) + gather_bufs(dt)
        + reduce_bufs(ds) + gather_bufs(ds)
        + reduce_bufs(fs) + gather_bufs(fs)
        + gather_bufs(fs) + gather_bufs(fs)
        + [vm((tokens, fs), F32)] * 2
        + [vm((tokens, fs), BF)] * 2
        + [
            pltpu.SemaphoreType.DMA((9,)),
            pltpu.SemaphoreType.DMA((6,)),
            pltpu.SemaphoreType.DMA((12,)),
            pltpu.SemaphoreType.DMA((12,)),
        ]
    )
    shapes = [(tokens, c) for c in (fs, ds, dt, ds, fs, fs)]
    hidden, features, signal, feature_grad, gate_signal, up_signal = pl.pallas_call(
        functools.partial(kernel, lax.axis_size("tc")),
        out_shape=[jax.ShapeDtypeStruct(s, BF) for s in shapes],
        in_specs=[pl.BlockSpec(memory_space=pl.ANY)] * 9,
        out_specs=[pl.BlockSpec(memory_space=pl.ANY)] * 6,
        scratch_shapes=scratch,
        compiler_params=pltpu.CompilerParams(
            collective_id=0, has_side_effects=True
        ),
        name="chain",
    )(*arguments)
    operands = (student_input, gate_signal, up_signal, hidden, feature_grad, features, signal)
    results = [(ds, fs), (ds, fs), (fs, ds), (ds, dt)]
    return pl.pallas_call(
        gradients,
        out_shape=[jax.ShapeDtypeStruct(s, F32) for s in results],
        in_specs=[pl.BlockSpec(memory_space=pl.ANY)] * 7,
        out_specs=[pl.BlockSpec(memory_space=pl.ANY)] * 4,
        scratch_shapes=[vm(a.shape, a.dtype) for a in operands]
        + [vm(s, F32) for s in results]
        + [pltpu.SemaphoreType.DMA((7,)), pltpu.SemaphoreType.DMA((4,))],
        name="gradients",
    )(*operands)


def solution(mesh):
    in_specs = (
        P(None, "st"),
        P(None, ("tr", "tc")),
        P("st", ("tr", "tc")),
        P(None, "st"),
        P(None, "st"),
        P("st", ("tr", "tc")),
        P("st", ("tr", "tc")),
        P(("tr", "tc"), "st"),
        P("st", ("tr", "tc")),
    )
    out_specs = (
        P("st", ("tr", "tc")),
        P("st", ("tr", "tc")),
        P(("tr", "tc"), "st"),
        P("st", ("tr", "tc")),
    )
    return jax.shard_map(body, mesh=mesh, in_specs=in_specs, out_specs=out_specs, check_vma=False)
```

```python
import functools
import math

import jax
import jax.numpy as jnp
from jax import lax
from jax.experimental import pallas as pl
from jax.experimental.pallas import tpu as pltpu
from jax.sharding import PartitionSpec as P

BF = jnp.bfloat16
F32 = jnp.float32
MESH = pl.DeviceIdType.MESH
N = 16
OTHERS = N - 1
FIRST = ((0, 256), (256, 256), (512, 256), (768, 128))
SECOND = ((0, 384), (384, 384), (768, 128))


def dot(a, b):
    return jnp.dot(a, b, preferred_element_type=F32)


def dot_cols(a, b):
    return lax.dot_general(a, b, (((1,), (1,)), ((), ())), preferred_element_type=F32)


def contract_rows(left, right):
    return lax.dot_general(
        left, right, (((0,), (0,)), ((), ())), preferred_element_type=F32
    )


def kernel(
    tc_size,
    th, res, td, xin, stream, wg, wu, wd, hd,
    o_hid, o_feat, o_sig, o_fg, o_gs, o_us,
    v_th, v_res, v_td, v_x, v_stream, v_wg, v_wu, v_wd, v_hd,
    f3, p3, r3, g3s, g3, f4, p4, r4, g5s, g5, f6, p6, r6, g6s, g6,
    gates, gate_ref, ups, up_ref, by_gate, by_up, s_gate, s_up,
    load_sem, out_sem, send_sem, recv_sem, *blocks,
):
    first, second = FIRST, SECOND
    take = lambda n: [blocks.pop(0) for _ in range(n)]
    blocks = list(blocks)
    n1, n2 = len(first), len(second)
    parts1 = list(zip(take(n1), take(n1)))
    lands1, pairs1, slots1, shares1, g2 = [take(n1) for _ in range(5)]
    parts7 = list(zip(take(n2), take(n2)))
    lands7, pairs7, slots7, shares7, g8 = [take(n2) for _ in range(5)]

    tokens = p3.shape[0]
    rows = tokens // N
    fs = wg.shape[1]
    st = lax.axis_index("st")
    grp = lax.axis_index("tr") * tc_size + lax.axis_index("tc")

    def st_peer(k):
        p = lax.rem(st + k, N)
        return p, {"st": p}

    def grp_peer(k):
        p = lax.rem(grp + k, N)
        return p, {"tr": p // tc_size, "tc": lax.rem(p, tc_size)}

    def at_rows(ref, i):
        return ref.at[pl.ds(pl.multiple_of(i * rows, rows), rows), :]

    loads = [
        pltpu.make_async_copy(src, dst, load_sem.at[i])
        for i, (src, dst) in enumerate(
            [
                (xin, v_x), (wg, v_wg), (wu, v_wu), (th, v_th), (td, v_td),
                (wd, v_wd), (hd, v_hd), (at_rows(stream, grp), v_stream),
                (at_rows(res, st), v_res),
            ]
        )
    ]
    for c in loads:
        c.start()

    barrier = pltpu.get_barrier_semaphore()

    def greet(k, carry):
        for peer in (st_peer, grp_peer):
            pl.semaphore_signal(barrier, inc=1, device_id=peer(k)[1], device_id_type=MESH)
        return carry

    lax.fori_loop(1, N, greet, 0)

    zs = N // 2
    z = lax.rem(st, zs)
    base = st - z
    across = {"st": lax.rem(st + zs, N)}
    half = zs * rows
    mine = pl.ds(pl.multiple_of(base * rows, half), half)
    theirs = pl.ds(pl.multiple_of((zs - base) * rows, half), half)
    owed = []

    def turn(like):
        owed.append(like)
        return len(owed) - 1

    def send(i, src, dst, device):
        pltpu.make_async_remote_copy(
            src_ref=src, dst_ref=dst,
            send_sem=send_sem.at[i], recv_sem=recv_sem.at[i],
            device_id=device, device_id_type=MESH,
        ).start()

    def each(first, last, fn):
        def one(k, carry):
            fn(k)
            return carry

        lax.fori_loop(first, last, one, 0)

    def await_in(i, like):
        pltpu.make_async_copy(like, like, recv_sem.at[i]).wait()

    def scatter(peer, part, slots):
        i = turn(slots)

        def one(k):
            p, device = peer(k)
            send(i, at_rows(part, p), slots.at[OTHERS - k], device)

        each(1, N, one)
        return i

    def summed(i, own, slots):
        await_in(i, slots)
        total = own
        for k in range(slots.shape[0]):
            total = total + slots[k].astype(F32)
        return total

    def spread(peer, share, whole, me):
        i = turn(whole.at[pl.ds(0, OTHERS * rows), :])
        each(1, N, lambda k: send(i, share, at_rows(whole, me), peer(k)[1]))
        return i

    def gathered(i):
        await_in(i, owed[i])

    def swap(part, land):
        i = turn(land)
        send(i, part.at[theirs, :], land, across)
        return i

    def z_peer(k):
        p = lax.rem(z + k, zs)
        return p, {"st": base + p}

    def z_scatter(part, slots):
        i = turn(slots)

        def one(k):
            p, device = z_peer(k)
            send(i, at_rows(part, p), slots.at[zs - 1 - k], device)

        each(1, zs, one)
        return i

    def z_spread(share, whole, me):
        i = turn(whole.at[pl.ds(0, (zs - 1) * rows), :])
        each(1, zs, lambda k: send(i, share, at_rows(whole, me), z_peer(k)[1]))
        return i

    def forward(whole):
        i = turn(whole.at[pl.ds(0, half), :])
        send(i, whole.at[mine, :], whole.at[mine, :], across)
        return i

    def put(ref, i, value):
        ref[pl.ds(pl.multiple_of(i * rows, rows), rows), :] = value

    def get(ref, i):
        return ref[pl.ds(pl.multiple_of(i * rows, rows), rows), :]

    def reduced(parts, lands, pairs, slots, finish, shares, wholes):
        turns = [swap(p, land) for (_, p), land in zip(parts, lands)]
        last = len(parts) - 1
        for n, (f, _) in enumerate(parts):
            await_in(turns[n], lands[n])
            pairs[n][...] = (f[mine, :] + lands[n][...].astype(F32)).astype(BF)
            turns[n] = z_scatter(pairs[n], slots[n])
        for n, (f, _) in enumerate(parts):
            own = get(f, st) + get(lands[n], z).astype(F32)
            share = finish(n, summed(turns[n], own, slots[n]))
            shares[n][...] = share
            if n < last:
                turns[n] = z_spread(shares[n], wholes[n], st)
            else:
                turns[n] = spread(st_peer, shares[n], wholes[n], st)
            put(wholes[n], st, share)
        for n in range(last):
            gathered(turns[n])
            turns[n] = forward(wholes[n])
        for i in turns:
            gathered(i)

    outs = []

    def out(src, dst):
        c = pltpu.make_async_copy(src, dst, out_sem.at[len(outs)])
        c.start()
        outs.append(c)

    for c in loads[:3]:
        c.wait()
    for (f, p), (at, w) in zip(parts1, first):
        cols = pl.ds(at, w)
        part = jnp.concatenate([dot(v_x[...], v_wg[:, cols]), dot(v_x[...], v_wu[:, cols])], axis=1)
        f[...] = part
        p[...] = part.astype(BF)
    for c in loads[3:]:
        c.wait()
    f4[...] = dot(v_th[...], v_td[...])
    pl.semaphore_wait(barrier, 2 * OTHERS)

    def finish_hidden(n, both):
        at, w = first[n]
        gate, up = both[:, :w], both[:, w:]
        gates[:, pl.ds(at, w)] = gate.astype(BF)
        ups[:, pl.ds(at, w)] = up.astype(BF)
        return (gate * jax.nn.sigmoid(gate) * up).astype(BF)

    reduced(parts1, lands1, pairs1, slots1, finish_hidden, shares1, g2)
    part = 0.0
    for g, (at, w) in zip(g2, first):
        part += dot(g[...], v_wd[pl.ds(at, w), :])
    f3[...] = part
    p3[...] = part.astype(BF)
    i = scatter(grp_peer, p3, r3)
    put(gate_ref, st, gates[...])
    put(up_ref, st, ups[...])
    i_gate = spread(st_peer, gates, gate_ref, st)
    for g, (at, w) in zip(g2, first):
        out(g, o_hid.at[:, pl.ds(at, w)])
    total = summed(i, get(f3, grp), r3)
    share = (v_stream[...].astype(F32) + total).astype(BF)
    g3s[...] = share
    i = spread(grp_peer, g3s, g3, grp)
    put(g3, grp, share)
    gathered(i)
    part = dot(g3[...], v_hd[...]) - f4[...]
    f4[...] = part
    p4[...] = part.astype(BF)
    i = scatter(st_peer, p4, r4)
    out(g3, o_feat)
    total = summed(i, get(f4, st), r4)
    share = ((total - v_res[...].astype(F32)) * (1.0 / math.sqrt(tokens))).astype(BF)
    g5s[...] = share
    i = spread(st_peer, g5s, g5, st)
    put(g5, st, share)
    gathered(i)
    part = dot_cols(g5[...], v_hd[...])
    f6[...] = part
    p6[...] = part.astype(BF)
    i = scatter(grp_peer, p6, r6)
    i_up = spread(st_peer, ups, up_ref, st)
    out(g5, o_sig)
    share = summed(i, get(f6, grp), r6).astype(BF)
    g6s[...] = share
    i = spread(grp_peer, g6s, g6, grp)
    put(g6, grp, share)
    gathered(i)
    for (f, p), (at, w) in zip(parts7, second):
        part = dot_cols(g6[...], v_wd[pl.ds(at, w), :])
        f[...] = part
        p[...] = part.astype(BF)
    out(g6, o_fg)

    def finish_grad(n, total):
        if n == 0:
            gathered(i_gate)
            gathered(i_up)
            gate = gate_ref[...].astype(F32)
            sigma = jax.nn.sigmoid(gate)
            by_gate[...] = up_ref[...].astype(F32) * (sigma * (1.0 + gate * (1.0 - sigma)))
            by_up[...] = gate * sigma
        return total.astype(BF)

    reduced(parts7, lands7, pairs7, slots7, finish_grad, shares7, g8)
    for made, by, dest in ((s_gate, by_gate, o_gs), (s_up, by_up, o_us)):
        for g, (at, w) in zip(g8, second):
            cols = pl.ds(at, w)
            made[:, cols] = (g[...].astype(F32) * by[:, cols]).astype(BF)
        out(made, dest)
    for i, like in enumerate(owed):
        pltpu.make_async_copy(like, like, send_sem.at[i]).wait()
    for c in outs:
        c.wait()


def gradients(
    x, gs, us, hid, fg, feat, sig, o_gate, o_up, o_down, o_head,
    v_x, v_gs, v_us, v_hid, v_fg, v_feat, v_sig, r_gate, r_up, r_down, r_head,
    load_sem, out_sem,
):
    pairs = [
        (feat, v_feat), (sig, v_sig), (hid, v_hid), (fg, v_fg),
        (x, v_x), (gs, v_gs), (us, v_us),
    ]
    loads = [
        pltpu.make_async_copy(src, dst, load_sem.at[i]) for i, (src, dst) in enumerate(pairs)
    ]
    for c in loads:
        c.start()
    stores = []
    for need, left, right, result, dest in (
        (2, v_feat, v_sig, r_head, o_head),
        (2, v_hid, v_fg, r_down, o_down),
        (2, v_x, v_gs, r_gate, o_gate),
        (1, v_x, v_us, r_up, o_up),
    ):
        for c in loads[:need]:
            c.wait()
        loads = loads[need:]
        result[...] = contract_rows(left[...], right[...])
        c = pltpu.make_async_copy(result, dest, out_sem.at[len(stores)])
        c.start()
        stores.append(c)
    for c in stores:
        c.wait()


def body(
    teacher_hidden, teacher_residual, teacher_down, student_input, student_stream,
    student_gate, student_up, student_down, head,
):
    tokens, ds = student_input.shape
    fs = student_gate.shape[1]
    dt = head.shape[1]
    rows = tokens // N
    arguments = (
        teacher_hidden, teacher_residual, teacher_down, student_input, student_stream,
        student_gate, student_up, student_down, head,
    )
    vm = lambda shape, dtype: pltpu.VMEM(shape, dtype)

    def reduce_bufs(cols):
        return [vm((tokens, cols), F32), vm((tokens, cols), BF), vm((OTHERS, rows, cols), BF)]

    def gather_bufs(cols):
        return [vm((rows, cols), BF), vm((tokens, cols), BF)]

    def block_bufs(cuts, of):
        wide = [w * of for _, w in cuts]
        return (
            [vm((tokens, w), F32) for w in wide]
            + [vm((tokens, w), BF) for w in wide]
            + [vm((tokens // 2, w), BF) for w in wide]
            + [vm((tokens // 2, w), BF) for w in wide]
            + [vm((N // 2 - 1, rows, w), BF) for w in wide]
            + [vm((rows, w), BF) for _, w in cuts]
            + [vm((tokens, w), BF) for _, w in cuts]
        )

    staged = [
        vm((rows, a.shape[1]), a.dtype) if i in (1, 4) else vm(a.shape, a.dtype)
        for i, a in enumerate(arguments)
    ]
    scratch = (
        staged
        + reduce_bufs(ds) + gather_bufs(ds)
        + reduce_bufs(dt) + gather_bufs(dt)
        + reduce_bufs(ds) + gather_bufs(ds)
        + gather_bufs(fs) + gather_bufs(fs)
        + [vm((tokens, fs), F32)] * 2
        + [vm((tokens, fs), BF)] * 2
        + [
            pltpu.SemaphoreType.DMA((9,)),
            pltpu.SemaphoreType.DMA((12,)),
            pltpu.SemaphoreType.DMA((48,)),
            pltpu.SemaphoreType.DMA((48,)),
        ]
        + block_bufs(FIRST, 2) + block_bufs(SECOND, 1)
    )
    shapes = [(tokens, c) for c in (fs, ds, dt, ds, fs, fs)]
    hidden, features, signal, feature_grad, gate_signal, up_signal = pl.pallas_call(
        functools.partial(kernel, lax.axis_size("tc")),
        out_shape=[jax.ShapeDtypeStruct(s, BF) for s in shapes],
        in_specs=[pl.BlockSpec(memory_space=pl.ANY)] * 9,
        out_specs=[pl.BlockSpec(memory_space=pl.ANY)] * 6,
        scratch_shapes=scratch,
        compiler_params=pltpu.CompilerParams(
            collective_id=0, has_side_effects=True
        ),
        name="chain",
    )(*arguments)
    operands = (student_input, gate_signal, up_signal, hidden, feature_grad, features, signal)
    results = [(ds, fs), (ds, fs), (fs, ds), (ds, dt)]
    return pl.pallas_call(
        gradients,
        out_shape=[jax.ShapeDtypeStruct(s, F32) for s in results],
        in_specs=[pl.BlockSpec(memory_space=pl.ANY)] * 7,
        out_specs=[pl.BlockSpec(memory_space=pl.ANY)] * 4,
        scratch_shapes=[vm(a.shape, a.dtype) for a in operands]
        + [vm(s, F32) for s in results]
        + [pltpu.SemaphoreType.DMA((7,)), pltpu.SemaphoreType.DMA((4,))],
        name="gradients",
    )(*operands)


def solution(mesh):
    in_specs = (
        P(None, "st"),
        P(None, ("tr", "tc")),
        P("st", ("tr", "tc")),
        P(None, "st"),
        P(None, "st"),
        P("st", ("tr", "tc")),
        P("st", ("tr", "tc")),
        P(("tr", "tc"), "st"),
        P("st", ("tr", "tc")),
    )
    out_specs = (
        P("st", ("tr", "tc")),
        P("st", ("tr", "tc")),
        P(("tr", "tc"), "st"),
        P("st", ("tr", "tc")),
    )
    return jax.shard_map(body, mesh=mesh, in_specs=in_specs, out_specs=out_specs, check_vma=False)
```

```python
import functools
import math

import jax
import jax.numpy as jnp
from jax import lax
from jax.experimental import pallas as pl
from jax.experimental.pallas import tpu as pltpu
from jax.sharding import PartitionSpec as P

BF = jnp.bfloat16
F32 = jnp.float32
MESH = pl.DeviceIdType.MESH
N = 16
OTHERS = N - 1
FIRST = ((0, 256), (256, 256), (512, 256), (768, 128))
SECOND = ((0, 384), (384, 384), (768, 128))


def dot(a, b):
    return jnp.dot(a, b, preferred_element_type=F32)


def dot_cols(a, b):
    return lax.dot_general(a, b, (((1,), (1,)), ((), ())), preferred_element_type=F32)


def contract_rows(left, right):
    return lax.dot_general(
        left, right, (((0,), (0,)), ((), ())), preferred_element_type=F32
    )


def kernel(
    tc_size,
    th, res, td, xin, stream, wg, wu, wd, hd,
    o_hid, o_feat, o_sig, o_fg, o_gs, o_us,
    v_th, v_res, v_td, v_x, v_stream, v_wg, v_wu, v_wd, v_hd,
    f3, p3, r3, g3s, g3, f4, p4, r4, g5s, g5, f6, p6, r6, g6s, g6,
    gates, gate_ref, ups, up_ref, by_gate, by_up, s_gate, s_up,
    load_sem, out_sem, send_sem, recv_sem, *blocks,
):
    first, second = FIRST, SECOND
    take = lambda n: [blocks.pop(0) for _ in range(n)]
    blocks = list(blocks)
    n1, n2 = len(first), len(second)
    parts1 = list(zip(take(n1), take(n1)))
    lands1, pairs1, slots1, shares1, g2 = [take(n1) for _ in range(5)]
    parts7 = list(zip(take(n2), take(n2)))
    lands7, pairs7, slots7, shares7, g8 = [take(n2) for _ in range(5)]

    tokens = p3.shape[0]
    rows = tokens // N
    fs = wg.shape[1]
    st = lax.axis_index("st")
    grp = lax.axis_index("tr") * tc_size + lax.axis_index("tc")

    zs = N // 2
    z = lax.rem(st, zs)
    base = st - z

    def from_far(k, length):
        k = k + 1
        return length // 2 + (k // 2) * (2 * lax.rem(k, 2) - 1)

    def z_peer(k):
        p = lax.rem(z + from_far(k, zs), zs)
        return base + p, {"st": base + p}, p

    def st_peer(k):
        p = z_peer(k // 2)[2]
        p = p + lax.rem(base + zs * (1 - lax.rem(k, 2)), N)
        return p, {"st": p}

    def grp_peer(k):
        trs = N // tc_size
        tr, tc = lax.axis_index("tr"), lax.axis_index("tc")
        tr = lax.rem(tr + from_far(lax.rem(k, N // 2) // 2, trs), trs)
        y, core = tc // 2 + 1 - k // (N // 2), tc + 1 - lax.rem(k, 2)
        tc = 2 * lax.rem(y, 2) + lax.rem(core, 2)
        return tr * tc_size + tc, {"tr": tr, "tc": tc}

    def at_rows(ref, i):
        return ref.at[pl.ds(pl.multiple_of(i * rows, rows), rows), :]

    loads = [
        pltpu.make_async_copy(src, dst, load_sem.at[i])
        for i, (src, dst) in enumerate(
            [
                (xin, v_x), (wg, v_wg), (wu, v_wu), (th, v_th), (td, v_td),
                (wd, v_wd), (hd, v_hd), (at_rows(stream, grp), v_stream),
                (at_rows(res, st), v_res),
            ]
        )
    ]
    for c in loads:
        c.start()

    barrier = pltpu.get_barrier_semaphore()

    def greet(k, carry):
        for peer in (st_peer, grp_peer):
            pl.semaphore_signal(barrier, inc=1, device_id=peer(k)[1], device_id_type=MESH)
        return carry

    lax.fori_loop(0, OTHERS, greet, 0)

    across = {"st": lax.rem(st + zs, N)}
    half = zs * rows
    mine = pl.ds(pl.multiple_of(base * rows, half), half)
    theirs = pl.ds(pl.multiple_of((zs - base) * rows, half), half)
    owed = []

    def turn(like):
        owed.append(like)
        return len(owed) - 1

    def send(i, src, dst, device):
        pltpu.make_async_remote_copy(
            src_ref=src, dst_ref=dst,
            send_sem=send_sem.at[i], recv_sem=recv_sem.at[i],
            device_id=device, device_id_type=MESH,
        ).start()

    def each(count, fn):
        def one(k, carry):
            fn(k)
            return carry

        lax.fori_loop(0, count, one, 0)

    def await_in(i, like):
        pltpu.make_async_copy(like, like, recv_sem.at[i]).wait()

    def scatter(peer, part, slots):
        i = turn(slots)

        def one(k):
            p, device = peer(k)
            send(i, at_rows(part, p), slots.at[k], device)

        each(OTHERS, one)
        return i

    def summed(i, own, slots):
        await_in(i, slots)
        total = own
        for k in range(slots.shape[0]):
            total = total + slots[k].astype(F32)
        return total

    def spread(peer, share, whole, me):
        i = turn(whole.at[pl.ds(0, OTHERS * rows), :])
        each(OTHERS, lambda k: send(i, share, at_rows(whole, me), peer(k)[1]))
        return i

    def gathered(i):
        await_in(i, owed[i])

    def swap(part, land):
        i = turn(land)
        send(i, part.at[theirs, :], land, across)
        return i

    def z_scatter(part, slots):
        i = turn(slots)

        def one(k):
            _, device, p = z_peer(k)
            send(i, at_rows(part, p), slots.at[k], device)

        each(zs - 1, one)
        return i

    def z_spread(share, whole, me):
        i = turn(whole.at[pl.ds(0, (zs - 1) * rows), :])
        each(zs - 1, lambda k: send(i, share, at_rows(whole, me), z_peer(k)[1]))
        return i

    def forward(whole):
        i = turn(whole.at[pl.ds(0, half), :])
        send(i, whole.at[mine, :], whole.at[mine, :], across)
        return i

    def put(ref, i, value):
        ref[pl.ds(pl.multiple_of(i * rows, rows), rows), :] = value

    def get(ref, i):
        return ref[pl.ds(pl.multiple_of(i * rows, rows), rows), :]

    def reduced(parts, lands, pairs, slots, finish, shares, wholes):
        turns = [swap(p, land) for (_, p), land in zip(parts, lands)]
        last = len(parts) - 1
        for n, (f, _) in enumerate(parts):
            await_in(turns[n], lands[n])
            pairs[n][...] = (f[mine, :] + lands[n][...].astype(F32)).astype(BF)
            turns[n] = z_scatter(pairs[n], slots[n])
        for n, (f, _) in enumerate(parts):
            own = get(f, st) + get(lands[n], z).astype(F32)
            share = finish(n, summed(turns[n], own, slots[n]))
            shares[n][...] = share
            if n < last:
                turns[n] = z_spread(shares[n], wholes[n], st)
            else:
                turns[n] = spread(st_peer, shares[n], wholes[n], st)
            put(wholes[n], st, share)
        for n in range(last):
            gathered(turns[n])
            turns[n] = forward(wholes[n])
        for i in turns:
            gathered(i)

    outs = []

    def out(src, dst):
        c = pltpu.make_async_copy(src, dst, out_sem.at[len(outs)])
        c.start()
        outs.append(c)

    for c in loads[:3]:
        c.wait()
    for (f, p), (at, w) in zip(parts1, first):
        cols = pl.ds(at, w)
        part = jnp.concatenate([dot(v_x[...], v_wg[:, cols]), dot(v_x[...], v_wu[:, cols])], axis=1)
        f[...] = part
        p[...] = part.astype(BF)
    for c in loads[3:]:
        c.wait()
    f4[...] = dot(v_th[...], v_td[...])
    pl.semaphore_wait(barrier, 2 * OTHERS)

    def finish_hidden(n, both):
        at, w = first[n]
        gate, up = both[:, :w], both[:, w:]
        gates[:, pl.ds(at, w)] = gate.astype(BF)
        ups[:, pl.ds(at, w)] = up.astype(BF)
        return (gate * jax.nn.sigmoid(gate) * up).astype(BF)

    reduced(parts1, lands1, pairs1, slots1, finish_hidden, shares1, g2)
    part = 0.0
    for g, (at, w) in zip(g2, first):
        part += dot(g[...], v_wd[pl.ds(at, w), :])
    f3[...] = part
    p3[...] = part.astype(BF)
    i = scatter(grp_peer, p3, r3)
    put(gate_ref, st, gates[...])
    put(up_ref, st, ups[...])
    i_gate = spread(st_peer, gates, gate_ref, st)
    for g, (at, w) in zip(g2, first):
        out(g, o_hid.at[:, pl.ds(at, w)])
    total = summed(i, get(f3, grp), r3)
    share = (v_stream[...].astype(F32) + total).astype(BF)
    g3s[...] = share
    i = spread(grp_peer, g3s, g3, grp)
    put(g3, grp, share)
    gathered(i)
    part = dot(g3[...], v_hd[...]) - f4[...]
    f4[...] = part
    p4[...] = part.astype(BF)
    i = scatter(st_peer, p4, r4)
    out(g3, o_feat)
    total = summed(i, get(f4, st), r4)
    share = ((total - v_res[...].astype(F32)) * (1.0 / math.sqrt(tokens))).astype(BF)
    g5s[...] = share
    i = spread(st_peer, g5s, g5, st)
    put(g5, st, share)
    gathered(i)
    part = dot_cols(g5[...], v_hd[...])
    f6[...] = part
    p6[...] = part.astype(BF)
    i = scatter(grp_peer, p6, r6)
    i_up = spread(st_peer, ups, up_ref, st)
    out(g5, o_sig)
    share = summed(i, get(f6, grp), r6).astype(BF)
    g6s[...] = share
    i = spread(grp_peer, g6s, g6, grp)
    put(g6, grp, share)
    gathered(i)
    for (f, p), (at, w) in zip(parts7, second):
        part = dot_cols(g6[...], v_wd[pl.ds(at, w), :])
        f[...] = part
        p[...] = part.astype(BF)
    out(g6, o_fg)

    def finish_grad(n, total):
        if n == 0:
            gathered(i_gate)
            gathered(i_up)
            gate = gate_ref[...].astype(F32)
            sigma = jax.nn.sigmoid(gate)
            by_gate[...] = up_ref[...].astype(F32) * (sigma * (1.0 + gate * (1.0 - sigma)))
            by_up[...] = gate * sigma
        return total.astype(BF)

    reduced(parts7, lands7, pairs7, slots7, finish_grad, shares7, g8)
    for made, by, dest in ((s_gate, by_gate, o_gs), (s_up, by_up, o_us)):
        for g, (at, w) in zip(g8, second):
            cols = pl.ds(at, w)
            made[:, cols] = (g[...].astype(F32) * by[:, cols]).astype(BF)
        out(made, dest)
    for i, like in enumerate(owed):
        pltpu.make_async_copy(like, like, send_sem.at[i]).wait()
    for c in outs:
        c.wait()


def gradients(
    x, gs, us, hid, fg, feat, sig, o_gate, o_up, o_down, o_head,
    v_x, v_gs, v_us, v_hid, v_fg, v_feat, v_sig, r_gate, r_up, r_down, r_head,
    load_sem, out_sem,
):
    pairs = [
        (feat, v_feat), (sig, v_sig), (hid, v_hid), (fg, v_fg),
        (x, v_x), (gs, v_gs), (us, v_us),
    ]
    loads = [
        pltpu.make_async_copy(src, dst, load_sem.at[i]) for i, (src, dst) in enumerate(pairs)
    ]
    for c in loads:
        c.start()
    stores = []
    for need, left, right, result, dest in (
        (2, v_feat, v_sig, r_head, o_head),
        (2, v_hid, v_fg, r_down, o_down),
        (2, v_x, v_gs, r_gate, o_gate),
        (1, v_x, v_us, r_up, o_up),
    ):
        for c in loads[:need]:
            c.wait()
        loads = loads[need:]
        result[...] = contract_rows(left[...], right[...])
        c = pltpu.make_async_copy(result, dest, out_sem.at[len(stores)])
        c.start()
        stores.append(c)
    for c in stores:
        c.wait()


def body(
    teacher_hidden, teacher_residual, teacher_down, student_input, student_stream,
    student_gate, student_up, student_down, head,
):
    tokens, ds = student_input.shape
    fs = student_gate.shape[1]
    dt = head.shape[1]
    rows = tokens // N
    arguments = (
        teacher_hidden, teacher_residual, teacher_down, student_input, student_stream,
        student_gate, student_up, student_down, head,
    )
    vm = lambda shape, dtype: pltpu.VMEM(shape, dtype)

    def reduce_bufs(cols):
        return [vm((tokens, cols), F32), vm((tokens, cols), BF), vm((OTHERS, rows, cols), BF)]

    def gather_bufs(cols):
        return [vm((rows, cols), BF), vm((tokens, cols), BF)]

    def block_bufs(cuts, of):
        wide = [w * of for _, w in cuts]
        return (
            [vm((tokens, w), F32) for w in wide]
            + [vm((tokens, w), BF) for w in wide]
            + [vm((tokens // 2, w), BF) for w in wide]
            + [vm((tokens // 2, w), BF) for w in wide]
            + [vm((N // 2 - 1, rows, w), BF) for w in wide]
            + [vm((rows, w), BF) for _, w in cuts]
            + [vm((tokens, w), BF) for _, w in cuts]
        )

    staged = [
        vm((rows, a.shape[1]), a.dtype) if i in (1, 4) else vm(a.shape, a.dtype)
        for i, a in enumerate(arguments)
    ]
    scratch = (
        staged
        + reduce_bufs(ds) + gather_bufs(ds)
        + reduce_bufs(dt) + gather_bufs(dt)
        + reduce_bufs(ds) + gather_bufs(ds)
        + gather_bufs(fs) + gather_bufs(fs)
        + [vm((tokens, fs), F32)] * 2
        + [vm((tokens, fs), BF)] * 2
        + [
            pltpu.SemaphoreType.DMA((9,)),
            pltpu.SemaphoreType.DMA((12,)),
            pltpu.SemaphoreType.DMA((48,)),
            pltpu.SemaphoreType.DMA((48,)),
        ]
        + block_bufs(FIRST, 2) + block_bufs(SECOND, 1)
    )
    shapes = [(tokens, c) for c in (fs, ds, dt, ds, fs, fs)]
    hidden, features, signal, feature_grad, gate_signal, up_signal = pl.pallas_call(
        functools.partial(kernel, lax.axis_size("tc")),
        out_shape=[jax.ShapeDtypeStruct(s, BF) for s in shapes],
        in_specs=[pl.BlockSpec(memory_space=pl.ANY)] * 9,
        out_specs=[pl.BlockSpec(memory_space=pl.ANY)] * 6,
        scratch_shapes=scratch,
        compiler_params=pltpu.CompilerParams(
            collective_id=0, has_side_effects=True
        ),
        name="chain",
    )(*arguments)
    operands = (student_input, gate_signal, up_signal, hidden, feature_grad, features, signal)
    results = [(ds, fs), (ds, fs), (fs, ds), (ds, dt)]
    return pl.pallas_call(
        gradients,
        out_shape=[jax.ShapeDtypeStruct(s, F32) for s in results],
        in_specs=[pl.BlockSpec(memory_space=pl.ANY)] * 7,
        out_specs=[pl.BlockSpec(memory_space=pl.ANY)] * 4,
        scratch_shapes=[vm(a.shape, a.dtype) for a in operands]
        + [vm(s, F32) for s in results]
        + [pltpu.SemaphoreType.DMA((7,)), pltpu.SemaphoreType.DMA((4,))],
        name="gradients",
    )(*operands)


def solution(mesh):
    in_specs = (
        P(None, "st"),
        P(None, ("tr", "tc")),
        P("st", ("tr", "tc")),
        P(None, "st"),
        P(None, "st"),
        P("st", ("tr", "tc")),
        P("st", ("tr", "tc")),
        P(("tr", "tc"), "st"),
        P("st", ("tr", "tc")),
    )
    out_specs = (
        P("st", ("tr", "tc")),
        P("st", ("tr", "tc")),
        P(("tr", "tc"), "st"),
        P("st", ("tr", "tc")),
    )
    return jax.shard_map(body, mesh=mesh, in_specs=in_specs, out_specs=out_specs, check_vma=False)
```

```python
import functools
import math

import jax
import jax.numpy as jnp
from jax import lax
from jax.experimental import pallas as pl
from jax.experimental.pallas import tpu as pltpu
from jax.sharding import PartitionSpec as P

BF = jnp.bfloat16
F32 = jnp.float32
MESH = pl.DeviceIdType.MESH
N = 16
OTHERS = N - 1
FIRST = ((0, 256), (256, 256), (512, 256), (768, 128))
SECOND = ((0, 256), (256, 256), (512, 256), (768, 128))
NARROW = ((0, 256),)
WIDE = ((0, 128), (128, 128), (256, 128), (384, 128))


def dot(a, b):
    return jnp.dot(a, b, preferred_element_type=F32)


def dot_cols(a, b):
    return lax.dot_general(a, b, (((1,), (1,)), ((), ())), preferred_element_type=F32)


def contract_rows(left, right):
    return lax.dot_general(
        left, right, (((0,), (0,)), ((), ())), preferred_element_type=F32
    )


def kernel(
    tc_size,
    th, res, td, xin, stream, wg, wu, wd, hd,
    o_hid, o_feat, o_sig, o_fg, o_gs, o_us,
    v_th, v_res, v_td, v_x, v_stream, v_wg, v_wu, v_wd, v_hd,
    f3, p3, g3s, g3, f4, p4, g5s, g5, f6, p6, g6s, g6,
    gates, gate_ref, ups, up_ref, by_gate, by_up, s_gate, s_up,
    load_sem, out_sem, send_sem, recv_sem, *blocks,
):
    first, second = FIRST, SECOND
    take = lambda n: [blocks.pop(0) for _ in range(n)]
    blocks = list(blocks)
    n1, n2 = len(first), len(second)
    parts1 = list(zip(take(n1), take(n1)))
    lands1, pairs1, slots1, shares1, g2 = [take(n1) for _ in range(5)]
    parts7 = list(zip(take(n2), take(n2)))
    lands7, pairs7, slots7, shares7, g8 = [take(n2) for _ in range(5)]
    r3, r4, r6 = take(len(NARROW)), take(len(WIDE)), take(len(NARROW))

    tokens = p3.shape[0]
    rows = tokens // N
    fs = wg.shape[1]
    st = lax.axis_index("st")
    grp = lax.axis_index("tr") * tc_size + lax.axis_index("tc")

    zs = N // 2
    z = lax.rem(st, zs)
    base = st - z

    def from_far(k, length):
        k = k + 1
        return length // 2 + (k // 2) * (2 * lax.rem(k, 2) - 1)

    def z_peer(k):
        p = lax.rem(z + from_far(k, zs), zs)
        return base + p, {"st": base + p}, p

    def st_peer(k):
        p = z_peer(k // 2)[2]
        p = p + lax.rem(base + zs * (1 - lax.rem(k, 2)), N)
        return p, {"st": p}

    def grp_peer(k):
        trs = N // tc_size
        tr, tc = lax.axis_index("tr"), lax.axis_index("tc")
        tr = lax.rem(tr + from_far(lax.rem(k, N // 2) // 2, trs), trs)
        y, core = tc // 2 + 1 - k // (N // 2), tc + 1 - lax.rem(k, 2)
        tc = 2 * lax.rem(y, 2) + lax.rem(core, 2)
        return tr * tc_size + tc, {"tr": tr, "tc": tc}

    def at_rows(ref, i):
        return ref.at[pl.ds(pl.multiple_of(i * rows, rows), rows), :]

    loads = [
        pltpu.make_async_copy(src, dst, load_sem.at[i])
        for i, (src, dst) in enumerate(
            [
                (xin, v_x), (wg, v_wg), (wu, v_wu), (th, v_th), (td, v_td),
                (wd, v_wd), (hd, v_hd), (at_rows(stream, grp), v_stream),
                (at_rows(res, st), v_res),
            ]
        )
    ]
    for c in loads:
        c.start()

    barrier = pltpu.get_barrier_semaphore()

    def greet(k, carry):
        for peer in (st_peer, grp_peer):
            pl.semaphore_signal(barrier, inc=1, device_id=peer(k)[1], device_id_type=MESH)
        return carry

    lax.fori_loop(0, OTHERS, greet, 0)

    across = {"st": lax.rem(st + zs, N)}
    half = zs * rows
    mine = pl.ds(pl.multiple_of(base * rows, half), half)
    theirs = pl.ds(pl.multiple_of((zs - base) * rows, half), half)
    owed = []

    def turn(like):
        owed.append(like)
        return len(owed) - 1

    def send(i, src, dst, device):
        pltpu.make_async_remote_copy(
            src_ref=src, dst_ref=dst,
            send_sem=send_sem.at[i], recv_sem=recv_sem.at[i],
            device_id=device, device_id_type=MESH,
        ).start()

    def each(count, fn):
        def one(k, carry):
            fn(k)
            return carry

        lax.fori_loop(0, count, one, 0)

    def await_in(i, like):
        pltpu.make_async_copy(like, like, recv_sem.at[i]).wait()

    def scatter(peer, part, slots):
        i = turn(slots)

        def one(k):
            p, device = peer(k)
            send(i, at_rows(part, p), slots.at[k], device)

        each(OTHERS, one)
        return i

    def summed(i, own, slots):
        await_in(i, slots)
        total = own
        for k in range(slots.shape[0]):
            total = total + slots[k].astype(F32)
        return total

    def spread(peer, share, whole, me):
        i = turn(whole.at[pl.ds(0, OTHERS * rows), :])
        each(OTHERS, lambda k: send(i, share, at_rows(whole, me), peer(k)[1]))
        return i

    def gathered(i):
        await_in(i, owed[i])

    def swap(part, land):
        i = turn(land)
        send(i, part.at[theirs, :], land, across)
        return i

    def z_scatter(part, slots):
        i = turn(slots)

        def one(k):
            _, device, p = z_peer(k)
            send(i, at_rows(part, p), slots.at[k], device)

        each(zs - 1, one)
        return i

    def z_spread(share, whole, me):
        i = turn(whole.at[pl.ds(0, (zs - 1) * rows), :])
        each(zs - 1, lambda k: send(i, share, at_rows(whole, me), z_peer(k)[1]))
        return i

    def forward(whole):
        i = turn(whole.at[pl.ds(0, half), :])
        send(i, whole.at[mine, :], whole.at[mine, :], across)
        return i

    def put(ref, i, value):
        ref[pl.ds(pl.multiple_of(i * rows, rows), rows), :] = value

    def get(ref, i):
        return ref[pl.ds(pl.multiple_of(i * rows, rows), rows), :]

    def direct(cuts, peer, me, total, part, slots, finish, share, whole, beside, behind):
        views = [pl.ds(at, w) for at, w in cuts]
        turns = [scatter(peer, part.at[:, v], b) for v, b in zip(views, slots)]
        beside()
        for n, v in enumerate(views):
            rows_here = pl.ds(pl.multiple_of(me * rows, rows), rows)
            made = finish(v, summed(turns[n], total[rows_here, v], slots[n]))
            share[:, v] = made
            turns[n] = spread(peer, share.at[:, v], whole.at[:, v], me)
            whole[rows_here, v] = made
        behind()
        for i in turns:
            gathered(i)

    def reduced(parts, lands, pairs, slots, finish, shares, wholes):
        turns = [swap(p, land) for (_, p), land in zip(parts, lands)]
        last = len(parts) - 1
        for n, (f, _) in enumerate(parts):
            await_in(turns[n], lands[n])
            pairs[n][...] = (f[mine, :] + lands[n][...].astype(F32)).astype(BF)
            turns[n] = z_scatter(pairs[n], slots[n])
        for n, (f, _) in enumerate(parts):
            own = get(f, st) + get(lands[n], z).astype(F32)
            share = finish(n, summed(turns[n], own, slots[n]))
            shares[n][...] = share
            if n < last:
                turns[n] = z_spread(shares[n], wholes[n], st)
            else:
                turns[n] = spread(st_peer, shares[n], wholes[n], st)
            put(wholes[n], st, share)
        for n in range(last):
            gathered(turns[n])
            turns[n] = forward(wholes[n])
        for i in turns:
            gathered(i)

    outs = []

    def out(src, dst):
        c = pltpu.make_async_copy(src, dst, out_sem.at[len(outs)])
        c.start()
        outs.append(c)

    for c in loads[:3]:
        c.wait()
    for (f, p), (at, w) in zip(parts1, first):
        cols = pl.ds(at, w)
        part = jnp.concatenate([dot(v_x[...], v_wg[:, cols]), dot(v_x[...], v_wu[:, cols])], axis=1)
        f[...] = part
        p[...] = part.astype(BF)
    for c in loads[3:]:
        c.wait()
    f4[...] = dot(v_th[...], v_td[...])
    pl.semaphore_wait(barrier, 2 * OTHERS)

    def finish_hidden(n, both):
        at, w = first[n]
        gate, up = both[:, :w], both[:, w:]
        gates[:, pl.ds(at, w)] = gate.astype(BF)
        ups[:, pl.ds(at, w)] = up.astype(BF)
        return (gate * jax.nn.sigmoid(gate) * up).astype(BF)

    reduced(parts1, lands1, pairs1, slots1, finish_hidden, shares1, g2)
    part = 0.0
    for g, (at, w) in zip(g2, first):
        part += dot(g[...], v_wd[pl.ds(at, w), :])
    f3[...] = part
    p3[...] = part.astype(BF)
    kept = {}

    def start(name, share, whole):
        put(whole, st, share[...])
        kept[name] = z_spread(share, whole, st)

    def pass_on(name, whole):
        gathered(kept[name])
        kept[name] = forward(whole)

    def beside_down():
        start("gate", gates, gate_ref)
        for g, (at, w) in zip(g2, first):
            out(g, o_hid.at[:, pl.ds(at, w)])

    def finish_features(v, total):
        return (v_stream[:, v].astype(F32) + total).astype(BF)

    direct(
        NARROW, grp_peer, grp, f3, p3, r3, finish_features, g3s, g3,
        beside_down, lambda: start("up", ups, up_ref),
    )
    part = dot(g3[...], v_hd[...]) - f4[...]
    f4[...] = part
    p4[...] = part.astype(BF)

    def finish_signal(v, total):
        return ((total - v_res[:, v].astype(F32)) * (1.0 / math.sqrt(tokens))).astype(BF)

    def beside_error():
        pass_on("gate", gate_ref)
        out(g3, o_feat)

    direct(
        WIDE, st_peer, st, f4, p4, r4, finish_signal, g5s, g5,
        beside_error, lambda: pass_on("up", up_ref),
    )
    part = dot_cols(g5[...], v_hd[...])
    f6[...] = part
    p6[...] = part.astype(BF)
    direct(
        NARROW, grp_peer, grp, f6, p6, r6, lambda v, total: total.astype(BF), g6s, g6,
        lambda: out(g5, o_sig), lambda: None,
    )
    for (f, p), (at, w) in zip(parts7, second):
        part = dot_cols(g6[...], v_wd[pl.ds(at, w), :])
        f[...] = part
        p[...] = part.astype(BF)
    out(g6, o_fg)

    def finish_grad(n, total):
        if n == 0:
            gathered(kept["gate"])
            gathered(kept["up"])
            gate = gate_ref[...].astype(F32)
            sigma = jax.nn.sigmoid(gate)
            by_gate[...] = up_ref[...].astype(F32) * (sigma * (1.0 + gate * (1.0 - sigma)))
            by_up[...] = gate * sigma
        return total.astype(BF)

    reduced(parts7, lands7, pairs7, slots7, finish_grad, shares7, g8)
    for made, by, dest in ((s_gate, by_gate, o_gs), (s_up, by_up, o_us)):
        for g, (at, w) in zip(g8, second):
            cols = pl.ds(at, w)
            made[:, cols] = (g[...].astype(F32) * by[:, cols]).astype(BF)
        out(made, dest)
    for i, like in enumerate(owed):
        pltpu.make_async_copy(like, like, send_sem.at[i]).wait()
    for c in outs:
        c.wait()


def gradients(
    x, gs, us, hid, fg, feat, sig, o_gate, o_up, o_down, o_head,
    v_x, v_gs, v_us, v_hid, v_fg, v_feat, v_sig, r_gate, r_up, r_down, r_head,
    load_sem, out_sem,
):
    pairs = [
        (feat, v_feat), (sig, v_sig), (hid, v_hid), (fg, v_fg),
        (x, v_x), (gs, v_gs), (us, v_us),
    ]
    loads = [
        pltpu.make_async_copy(src, dst, load_sem.at[i]) for i, (src, dst) in enumerate(pairs)
    ]
    for c in loads:
        c.start()
    stores = []
    for need, left, right, result, dest in (
        (2, v_feat, v_sig, r_head, o_head),
        (2, v_hid, v_fg, r_down, o_down),
        (2, v_x, v_gs, r_gate, o_gate),
        (1, v_x, v_us, r_up, o_up),
    ):
        for c in loads[:need]:
            c.wait()
        loads = loads[need:]
        result[...] = contract_rows(left[...], right[...])
        c = pltpu.make_async_copy(result, dest, out_sem.at[len(stores)])
        c.start()
        stores.append(c)
    for c in stores:
        c.wait()


def body(
    teacher_hidden, teacher_residual, teacher_down, student_input, student_stream,
    student_gate, student_up, student_down, head,
):
    tokens, ds = student_input.shape
    fs = student_gate.shape[1]
    dt = head.shape[1]
    rows = tokens // N
    arguments = (
        teacher_hidden, teacher_residual, teacher_down, student_input, student_stream,
        student_gate, student_up, student_down, head,
    )
    vm = lambda shape, dtype: pltpu.VMEM(shape, dtype)

    def reduce_bufs(cols):
        return [vm((tokens, cols), F32), vm((tokens, cols), BF)]

    def gather_bufs(cols):
        return [vm((rows, cols), BF), vm((tokens, cols), BF)]

    def block_bufs(cuts, of):
        wide = [w * of for _, w in cuts]
        return (
            [vm((tokens, w), F32) for w in wide]
            + [vm((tokens, w), BF) for w in wide]
            + [vm((tokens // 2, w), BF) for w in wide]
            + [vm((tokens // 2, w), BF) for w in wide]
            + [vm((N // 2 - 1, rows, w), BF) for w in wide]
            + [vm((rows, w), BF) for _, w in cuts]
            + [vm((tokens, w), BF) for _, w in cuts]
        )

    staged = [
        vm((rows, a.shape[1]), a.dtype) if i in (1, 4) else vm(a.shape, a.dtype)
        for i, a in enumerate(arguments)
    ]
    scratch = (
        staged
        + reduce_bufs(ds) + gather_bufs(ds)
        + reduce_bufs(dt) + gather_bufs(dt)
        + reduce_bufs(ds) + gather_bufs(ds)
        + gather_bufs(fs) + gather_bufs(fs)
        + [vm((tokens, fs), F32)] * 2
        + [vm((tokens, fs), BF)] * 2
        + [
            pltpu.SemaphoreType.DMA((9,)),
            pltpu.SemaphoreType.DMA((12,)),
            pltpu.SemaphoreType.DMA((48,)),
            pltpu.SemaphoreType.DMA((48,)),
        ]
        + block_bufs(FIRST, 2) + block_bufs(SECOND, 1)
        + [vm((OTHERS, rows, w), BF) for _, w in NARROW + WIDE + NARROW]
    )
    shapes = [(tokens, c) for c in (fs, ds, dt, ds, fs, fs)]
    hidden, features, signal, feature_grad, gate_signal, up_signal = pl.pallas_call(
        functools.partial(kernel, lax.axis_size("tc")),
        out_shape=[jax.ShapeDtypeStruct(s, BF) for s in shapes],
        in_specs=[pl.BlockSpec(memory_space=pl.ANY)] * 9,
        out_specs=[pl.BlockSpec(memory_space=pl.ANY)] * 6,
        scratch_shapes=scratch,
        compiler_params=pltpu.CompilerParams(
            collective_id=0, has_side_effects=True
        ),
        name="chain",
    )(*arguments)
    operands = (student_input, gate_signal, up_signal, hidden, feature_grad, features, signal)
    results = [(ds, fs), (ds, fs), (fs, ds), (ds, dt)]
    return pl.pallas_call(
        gradients,
        out_shape=[jax.ShapeDtypeStruct(s, F32) for s in results],
        in_specs=[pl.BlockSpec(memory_space=pl.ANY)] * 7,
        out_specs=[pl.BlockSpec(memory_space=pl.ANY)] * 4,
        scratch_shapes=[vm(a.shape, a.dtype) for a in operands]
        + [vm(s, F32) for s in results]
        + [pltpu.SemaphoreType.DMA((7,)), pltpu.SemaphoreType.DMA((4,))],
        name="gradients",
    )(*operands)


def solution(mesh):
    in_specs = (
        P(None, "st"),
        P(None, ("tr", "tc")),
        P("st", ("tr", "tc")),
        P(None, "st"),
        P(None, "st"),
        P("st", ("tr", "tc")),
        P("st", ("tr", "tc")),
        P(("tr", "tc"), "st"),
        P("st", ("tr", "tc")),
    )
    out_specs = (
        P("st", ("tr", "tc")),
        P("st", ("tr", "tc")),
        P(("tr", "tc"), "st"),
        P("st", ("tr", "tc")),
    )
    return jax.shard_map(body, mesh=mesh, in_specs=in_specs, out_specs=out_specs, check_vma=False)
```

```python
import functools
import math

import jax
import jax.numpy as jnp
from jax import lax
from jax.experimental import pallas as pl
from jax.experimental.pallas import tpu as pltpu
from jax.sharding import PartitionSpec as P

BF = jnp.bfloat16
F32 = jnp.float32
MESH = pl.DeviceIdType.MESH
N = 16
OTHERS = N - 1
FIRST = ((0, 256), (256, 256), (512, 128), (640, 128), (768, 128))
SECOND = ((0, 384), (384, 256), (640, 128), (768, 128))
NARROW = ((0, 256),)
WIDE = ((0, 128), (128, 128), (256, 128), (384, 128))


def dot(a, b):
    return jnp.dot(a, b, preferred_element_type=F32)


def dot_cols(a, b):
    return lax.dot_general(a, b, (((1,), (1,)), ((), ())), preferred_element_type=F32)


def contract_rows(left, right):
    return lax.dot_general(
        left, right, (((0,), (0,)), ((), ())), preferred_element_type=F32
    )


def kernel(
    tc_size,
    th, res, td, xin, stream, wg, wu, wd, hd,
    o_hid, o_feat, o_sig, o_fg, o_gs, o_us,
    v_th, v_res, v_td, v_x, v_stream, v_wg, v_wu, v_wd, v_hd,
    f3, p3, g3s, g3, f4, p4, g5s, g5, f6, p6, g6s, g6,
    gates, gate_ref, ups, up_ref, by_gate, by_up, s_gate, s_up,
    load_sem, out_sem, send_sem, recv_sem, *blocks,
):
    first, second = FIRST, SECOND
    take = lambda n: [blocks.pop(0) for _ in range(n)]
    blocks = list(blocks)
    n1, n2 = len(first), len(second)
    parts1 = list(zip(take(n1), take(n1)))
    lands1, pairs1, slots1, shares1, g2 = [take(n1) for _ in range(5)]
    parts7 = list(zip(take(n2), take(n2)))
    lands7, pairs7, slots7, shares7, g8 = [take(n2) for _ in range(5)]
    r3, r4, r6 = take(len(NARROW)), take(len(WIDE)), take(len(NARROW))

    tokens = p3.shape[0]
    rows = tokens // N
    fs = wg.shape[1]
    st = lax.axis_index("st")
    grp = lax.axis_index("tr") * tc_size + lax.axis_index("tc")

    zs = N // 2
    z = lax.rem(st, zs)
    base = st - z

    def from_far(k, length):
        k = k + 1
        return length // 2 + (k // 2) * (2 * lax.rem(k, 2) - 1)

    def z_peer(k):
        p = lax.rem(z + from_far(k, zs), zs)
        return base + p, {"st": base + p}, p

    def st_peer(k):
        p = z_peer(k // 2)[2]
        p = p + lax.rem(base + zs * (1 - lax.rem(k, 2)), N)
        return p, {"st": p}

    def grp_peer(k):
        trs = N // tc_size
        tr, tc = lax.axis_index("tr"), lax.axis_index("tc")
        tr = lax.rem(tr + from_far(lax.rem(k, N // 2) // 2, trs), trs)
        y, core = tc // 2 + 1 - k // (N // 2), tc + 1 - lax.rem(k, 2)
        tc = 2 * lax.rem(y, 2) + lax.rem(core, 2)
        return tr * tc_size + tc, {"tr": tr, "tc": tc}

    def at_rows(ref, i):
        return ref.at[pl.ds(pl.multiple_of(i * rows, rows), rows), :]

    loads = [
        pltpu.make_async_copy(src, dst, load_sem.at[i])
        for i, (src, dst) in enumerate(
            [
                (xin, v_x), (wg, v_wg), (wu, v_wu), (th, v_th), (td, v_td),
                (wd, v_wd), (hd, v_hd), (at_rows(stream, grp), v_stream),
                (at_rows(res, st), v_res),
            ]
        )
    ]
    for c in loads:
        c.start()

    barrier = pltpu.get_barrier_semaphore()

    def greet(k, carry):
        for peer in (st_peer, grp_peer):
            pl.semaphore_signal(barrier, inc=1, device_id=peer(k)[1], device_id_type=MESH)
        return carry

    lax.fori_loop(0, OTHERS, greet, 0)

    across = {"st": lax.rem(st + zs, N)}
    half = zs * rows
    mine = pl.ds(pl.multiple_of(base * rows, half), half)
    theirs = pl.ds(pl.multiple_of((zs - base) * rows, half), half)
    owed = []

    def turn(like):
        owed.append(like)
        return len(owed) - 1

    def send(i, src, dst, device):
        pltpu.make_async_remote_copy(
            src_ref=src, dst_ref=dst,
            send_sem=send_sem.at[i], recv_sem=recv_sem.at[i],
            device_id=device, device_id_type=MESH,
        ).start()

    def each(count, fn):
        def one(k, carry):
            fn(k)
            return carry

        lax.fori_loop(0, count, one, 0)

    def await_in(i, like):
        pltpu.make_async_copy(like, like, recv_sem.at[i]).wait()

    def scatter(peer, part, slots):
        i = turn(slots)

        def one(k):
            p, device = peer(k)
            send(i, at_rows(part, p), slots.at[k], device)

        each(OTHERS, one)
        return i

    def summed(i, own, slots):
        await_in(i, slots)
        total = own
        for k in range(slots.shape[0]):
            total = total + slots[k].astype(F32)
        return total

    def spread(peer, share, whole, me):
        i = turn(whole.at[pl.ds(0, OTHERS * rows), :])
        each(OTHERS, lambda k: send(i, share, at_rows(whole, me), peer(k)[1]))
        return i

    def gathered(i):
        await_in(i, owed[i])

    def swap(part, land):
        i = turn(land)
        send(i, part.at[theirs, :], land, across)
        return i

    def z_scatter(part, slots):
        i = turn(slots)

        def one(k):
            _, device, p = z_peer(k)
            send(i, at_rows(part, p), slots.at[k], device)

        each(zs - 1, one)
        return i

    def z_spread(share, whole, me):
        i = turn(whole.at[pl.ds(0, (zs - 1) * rows), :])
        each(zs - 1, lambda k: send(i, share, at_rows(whole, me), z_peer(k)[1]))
        return i

    def forward(whole):
        i = turn(whole.at[pl.ds(0, half), :])
        send(i, whole.at[mine, :], whole.at[mine, :], across)
        return i

    def put(ref, i, value):
        ref[pl.ds(pl.multiple_of(i * rows, rows), rows), :] = value

    def get(ref, i):
        return ref[pl.ds(pl.multiple_of(i * rows, rows), rows), :]

    def direct(cuts, peer, me, total, part, slots, finish, share, whole, beside, behind):
        views = [pl.ds(at, w) for at, w in cuts]
        turns = [scatter(peer, part.at[:, v], b) for v, b in zip(views, slots)]
        beside()
        for n, v in enumerate(views):
            rows_here = pl.ds(pl.multiple_of(me * rows, rows), rows)
            made = finish(v, summed(turns[n], total[rows_here, v], slots[n]))
            share[:, v] = made
            turns[n] = spread(peer, share.at[:, v], whole.at[:, v], me)
            whole[rows_here, v] = made
        behind()
        for i in turns:
            gathered(i)

    def reduced(parts, lands, pairs, slots, finish, shares, wholes, ready=lambda n: None):
        turns = [None] + [swap(parts[1][1], lands[1])]
        turns[0] = scatter(st_peer, parts[0][1], slots[0])
        turns += [swap(p, land) for (_, p), land in zip(parts[2:], lands[2:])]
        last = len(parts) - 1
        for n, (f, _) in list(enumerate(parts))[1:]:
            await_in(turns[n], lands[n])
            pairs[n][...] = (f[mine, :] + lands[n][...].astype(F32)).astype(BF)
            turns[n] = z_scatter(pairs[n], slots[n])
        passed = 0
        for n, (f, _) in enumerate(parts):
            if n == last:
                gathered(turns[0])
                turns[0] = forward(wholes[0])
                passed = 1
            own = get(f, st)
            if n:
                own = own + get(lands[n], z).astype(F32)
            share = finish(n, summed(turns[n], own, slots[n]))
            shares[n][...] = share
            if n < last:
                turns[n] = z_spread(shares[n], wholes[n], st)
            else:
                turns[n] = spread(st_peer, shares[n], wholes[n], st)
            put(wholes[n], st, share)
        for n in range(passed, last):
            gathered(turns[n])
            turns[n] = forward(wholes[n])
        for n, i in enumerate(turns):
            gathered(i)
            ready(n)

    outs = []

    def out(src, dst):
        c = pltpu.make_async_copy(src, dst, out_sem.at[len(outs)])
        c.start()
        outs.append(c)

    for c in loads[:3]:
        c.wait()
    for (f, p), (at, w) in zip(parts1, first):
        cols = pl.ds(at, w)
        part = jnp.concatenate([dot(v_x[...], v_wg[:, cols]), dot(v_x[...], v_wu[:, cols])], axis=1)
        f[...] = part
        p[...] = part.astype(BF)
    for c in loads[3:]:
        c.wait()
    f4[...] = dot(v_th[...], v_td[...])
    pl.semaphore_wait(barrier, 2 * OTHERS)

    def finish_hidden(n, both):
        at, w = first[n]
        gate, up = both[:, :w], both[:, w:]
        gates[:, pl.ds(at, w)] = gate.astype(BF)
        ups[:, pl.ds(at, w)] = up.astype(BF)
        return (gate * jax.nn.sigmoid(gate) * up).astype(BF)

    reduced(parts1, lands1, pairs1, slots1, finish_hidden, shares1, g2)
    part = 0.0
    for g, (at, w) in zip(g2, first):
        part += dot(g[...], v_wd[pl.ds(at, w), :])
    f3[...] = part
    p3[...] = part.astype(BF)
    kept = {}

    def start(name, share, whole):
        put(whole, st, share[...])
        kept[name] = z_spread(share, whole, st)

    def pass_on(name, whole):
        gathered(kept[name])
        kept[name] = forward(whole)

    def beside_down():
        start("gate", gates, gate_ref)
        for g, (at, w) in zip(g2, first):
            out(g, o_hid.at[:, pl.ds(at, w)])

    def finish_features(v, total):
        return (v_stream[:, v].astype(F32) + total).astype(BF)

    direct(
        NARROW, grp_peer, grp, f3, p3, r3, finish_features, g3s, g3,
        beside_down, lambda: start("up", ups, up_ref),
    )
    part = dot(g3[...], v_hd[...]) - f4[...]
    f4[...] = part
    p4[...] = part.astype(BF)

    def finish_signal(v, total):
        return ((total - v_res[:, v].astype(F32)) * (1.0 / math.sqrt(tokens))).astype(BF)

    def beside_error():
        pass_on("gate", gate_ref)
        out(g3, o_feat)

    direct(
        WIDE, st_peer, st, f4, p4, r4, finish_signal, g5s, g5,
        beside_error, lambda: pass_on("up", up_ref),
    )
    part = dot_cols(g5[...], v_hd[...])
    f6[...] = part
    p6[...] = part.astype(BF)
    direct(
        NARROW, grp_peer, grp, f6, p6, r6, lambda v, total: total.astype(BF), g6s, g6,
        lambda: out(g5, o_sig), lambda: None,
    )
    for (f, p), (at, w) in zip(parts7, second):
        part = dot_cols(g6[...], v_wd[pl.ds(at, w), :])
        f[...] = part
        p[...] = part.astype(BF)
    out(g6, o_fg)

    def finish_grad(n, total):
        if n == 0:
            gathered(kept["gate"])
            gathered(kept["up"])
            gate = gate_ref[...].astype(F32)
            sigma = jax.nn.sigmoid(gate)
            by_gate[...] = up_ref[...].astype(F32) * (sigma * (1.0 + gate * (1.0 - sigma)))
            by_up[...] = gate * sigma
        return total.astype(BF)

    def ready_grad(n):
        at, w = second[n]
        cols = pl.ds(at, w)
        grad = g8[n][...].astype(F32)
        for made, by, dest in ((s_gate, by_gate, o_gs), (s_up, by_up, o_us)):
            made[:, cols] = (grad * by[:, cols]).astype(BF)
            out(made.at[:, cols], dest.at[:, cols])

    reduced(parts7, lands7, pairs7, slots7, finish_grad, shares7, g8, ready_grad)
    for i, like in enumerate(owed):
        pltpu.make_async_copy(like, like, send_sem.at[i]).wait()
    for c in outs:
        c.wait()


def gradients(
    x, gs, us, hid, fg, feat, sig, o_gate, o_up, o_down, o_head,
    v_x, v_gs, v_us, v_hid, v_fg, v_feat, v_sig, r_gate, r_up, r_down, r_head,
    load_sem, out_sem,
):
    pairs = [
        (feat, v_feat), (sig, v_sig), (hid, v_hid), (fg, v_fg),
        (x, v_x), (gs, v_gs), (us, v_us),
    ]
    loads = [
        pltpu.make_async_copy(src, dst, load_sem.at[i]) for i, (src, dst) in enumerate(pairs)
    ]
    for c in loads:
        c.start()
    stores = []
    for need, left, right, result, dest in (
        (2, v_feat, v_sig, r_head, o_head),
        (2, v_hid, v_fg, r_down, o_down),
        (2, v_x, v_gs, r_gate, o_gate),
        (1, v_x, v_us, r_up, o_up),
    ):
        for c in loads[:need]:
            c.wait()
        loads = loads[need:]
        result[...] = contract_rows(left[...], right[...])
        c = pltpu.make_async_copy(result, dest, out_sem.at[len(stores)])
        c.start()
        stores.append(c)
    for c in stores:
        c.wait()


def body(
    teacher_hidden, teacher_residual, teacher_down, student_input, student_stream,
    student_gate, student_up, student_down, head,
):
    tokens, ds = student_input.shape
    fs = student_gate.shape[1]
    dt = head.shape[1]
    rows = tokens // N
    arguments = (
        teacher_hidden, teacher_residual, teacher_down, student_input, student_stream,
        student_gate, student_up, student_down, head,
    )
    vm = lambda shape, dtype: pltpu.VMEM(shape, dtype)

    def reduce_bufs(cols):
        return [vm((tokens, cols), F32), vm((tokens, cols), BF)]

    def gather_bufs(cols):
        return [vm((rows, cols), BF), vm((tokens, cols), BF)]

    def block_bufs(cuts, of):
        wide = [w * of for _, w in cuts]
        return (
            [vm((tokens, w), F32) for w in wide]
            + [vm((tokens, w), BF) for w in wide]
            + [vm((tokens // 2, w), BF) for w in wide]
            + [vm((tokens // 2, w), BF) for w in wide]
            + [vm((N // 2 - 1 if n else OTHERS, rows, w), BF) for n, w in enumerate(wide)]
            + [vm((rows, w), BF) for _, w in cuts]
            + [vm((tokens, w), BF) for _, w in cuts]
        )

    staged = [
        vm((rows, a.shape[1]), a.dtype) if i in (1, 4) else vm(a.shape, a.dtype)
        for i, a in enumerate(arguments)
    ]
    scratch = (
        staged
        + reduce_bufs(ds) + gather_bufs(ds)
        + reduce_bufs(dt) + gather_bufs(dt)
        + reduce_bufs(ds) + gather_bufs(ds)
        + gather_bufs(fs) + gather_bufs(fs)
        + [vm((tokens, fs), F32)] * 2
        + [vm((tokens, fs), BF)] * 2
        + [
            pltpu.SemaphoreType.DMA((9,)),
            pltpu.SemaphoreType.DMA((16,)),
            pltpu.SemaphoreType.DMA((48,)),
            pltpu.SemaphoreType.DMA((48,)),
        ]
        + block_bufs(FIRST, 2) + block_bufs(SECOND, 1)
        + [vm((OTHERS, rows, w), BF) for _, w in NARROW + WIDE + NARROW]
    )
    shapes = [(tokens, c) for c in (fs, ds, dt, ds, fs, fs)]
    hidden, features, signal, feature_grad, gate_signal, up_signal = pl.pallas_call(
        functools.partial(kernel, lax.axis_size("tc")),
        out_shape=[jax.ShapeDtypeStruct(s, BF) for s in shapes],
        in_specs=[pl.BlockSpec(memory_space=pl.ANY)] * 9,
        out_specs=[pl.BlockSpec(memory_space=pl.ANY)] * 6,
        scratch_shapes=scratch,
        compiler_params=pltpu.CompilerParams(
            collective_id=0, has_side_effects=True
        ),
        name="chain",
    )(*arguments)
    operands = (student_input, gate_signal, up_signal, hidden, feature_grad, features, signal)
    results = [(ds, fs), (ds, fs), (fs, ds), (ds, dt)]
    return pl.pallas_call(
        gradients,
        out_shape=[jax.ShapeDtypeStruct(s, F32) for s in results],
        in_specs=[pl.BlockSpec(memory_space=pl.ANY)] * 7,
        out_specs=[pl.BlockSpec(memory_space=pl.ANY)] * 4,
        scratch_shapes=[vm(a.shape, a.dtype) for a in operands]
        + [vm(s, F32) for s in results]
        + [pltpu.SemaphoreType.DMA((7,)), pltpu.SemaphoreType.DMA((4,))],
        name="gradients",
    )(*operands)


def solution(mesh):
    in_specs = (
        P(None, "st"),
        P(None, ("tr", "tc")),
        P("st", ("tr", "tc")),
        P(None, "st"),
        P(None, "st"),
        P("st", ("tr", "tc")),
        P("st", ("tr", "tc")),
        P(("tr", "tc"), "st"),
        P("st", ("tr", "tc")),
    )
    out_specs = (
        P("st", ("tr", "tc")),
        P("st", ("tr", "tc")),
        P(("tr", "tc"), "st"),
        P("st", ("tr", "tc")),
    )
    return jax.shard_map(body, mesh=mesh, in_specs=in_specs, out_specs=out_specs, check_vma=False)
```

```python
import functools
import math

import jax
import jax.numpy as jnp
from jax import lax
from jax.experimental import pallas as pl
from jax.experimental.pallas import tpu as pltpu
from jax.sharding import PartitionSpec as P

BF = jnp.bfloat16
F32 = jnp.float32
MESH = pl.DeviceIdType.MESH
N = 16
OTHERS = N - 1
FIRST = ((0, 256), (256, 128), (384, 128), (512, 128), (640, 128), (768, 128))
SECOND = ((0, 384), (384, 128), (512, 128), (640, 128), (768, 128))
NARROW = ((0, 256),)
WIDE = ((0, 128), (128, 128), (256, 128), (384, 128))


def dot(a, b):
    return jnp.dot(a, b, preferred_element_type=F32)


def dot_cols(a, b):
    return lax.dot_general(a, b, (((1,), (1,)), ((), ())), preferred_element_type=F32)


def contract_rows(left, right):
    return lax.dot_general(
        left, right, (((0,), (0,)), ((), ())), preferred_element_type=F32
    )


def kernel(
    tc_size,
    th, res, td, xin, stream, wg, wu, wd, hd,
    o_hid, o_feat, o_sig, o_fg, o_gs, o_us,
    v_th, v_res, v_td, v_x, v_stream, v_wg, v_wu, v_wd, v_hd,
    f3, p3, g3s, g3, f4, p4, g5s, g5, f6, p6, g6s, g6,
    gates, gate_ref, ups, up_ref, by_gate, by_up, s_gate, s_up,
    load_sem, out_sem, send_sem, recv_sem, *blocks,
):
    first, second = FIRST, SECOND
    take = lambda n: [blocks.pop(0) for _ in range(n)]
    blocks = list(blocks)
    n1, n2 = len(first), len(second)
    parts1 = list(zip(take(n1), take(n1)))
    lands1, pairs1, slots1, shares1, g2 = [take(n1) for _ in range(5)]
    parts7 = list(zip(take(n2), take(n2)))
    lands7, pairs7, slots7, shares7, g8 = [take(n2) for _ in range(5)]
    r3, r4, r6 = take(len(NARROW)), take(len(WIDE)), take(len(NARROW))

    tokens = p3.shape[0]
    rows = tokens // N
    fs = wg.shape[1]
    st = lax.axis_index("st")
    grp = lax.axis_index("tr") * tc_size + lax.axis_index("tc")

    zs = N // 2
    z = lax.rem(st, zs)
    base = st - z

    def from_far(k, length):
        k = k + 1
        return length // 2 + (k // 2) * (2 * lax.rem(k, 2) - 1)

    def z_peer(k):
        p = lax.rem(z + from_far(k, zs), zs)
        return base + p, {"st": base + p}, p

    def st_peer(k):
        p = z_peer(k // 2)[2]
        p = p + lax.rem(base + zs * (1 - lax.rem(k, 2)), N)
        return p, {"st": p}

    def grp_peer(k):
        trs = N // tc_size
        tr, tc = lax.axis_index("tr"), lax.axis_index("tc")
        tr = lax.rem(tr + from_far(lax.rem(k, N // 2) // 2, trs), trs)
        y, core = tc // 2 + 1 - k // (N // 2), tc + 1 - lax.rem(k, 2)
        tc = 2 * lax.rem(y, 2) + lax.rem(core, 2)
        return tr * tc_size + tc, {"tr": tr, "tc": tc}

    def at_rows(ref, i):
        return ref.at[pl.ds(pl.multiple_of(i * rows, rows), rows), :]

    loads = [
        pltpu.make_async_copy(src, dst, load_sem.at[i])
        for i, (src, dst) in enumerate(
            [
                (xin, v_x), (wg, v_wg), (wu, v_wu), (th, v_th), (td, v_td),
                (wd, v_wd), (hd, v_hd), (at_rows(stream, grp), v_stream),
                (at_rows(res, st), v_res),
            ]
        )
    ]
    for c in loads:
        c.start()

    barrier = pltpu.get_barrier_semaphore()

    def greet(k, carry):
        for peer in (st_peer, grp_peer):
            pl.semaphore_signal(barrier, inc=1, device_id=peer(k)[1], device_id_type=MESH)
        return carry

    lax.fori_loop(0, OTHERS, greet, 0)

    across = {"st": lax.rem(st + zs, N)}
    half = zs * rows
    mine = pl.ds(pl.multiple_of(base * rows, half), half)
    theirs = pl.ds(pl.multiple_of((zs - base) * rows, half), half)
    owed = []

    def turn(like):
        owed.append(like)
        return len(owed) - 1

    def send(i, src, dst, device):
        pltpu.make_async_remote_copy(
            src_ref=src, dst_ref=dst,
            send_sem=send_sem.at[i], recv_sem=recv_sem.at[i],
            device_id=device, device_id_type=MESH,
        ).start()

    def each(count, fn):
        def one(k, carry):
            fn(k)
            return carry

        lax.fori_loop(0, count, one, 0)

    def await_in(i, like):
        pltpu.make_async_copy(like, like, recv_sem.at[i]).wait()

    def scatter(peer, part, slots):
        i = turn(slots)

        def one(k):
            p, device = peer(k)
            send(i, at_rows(part, p), slots.at[k], device)

        each(OTHERS, one)
        return i

    def summed(i, own, slots):
        await_in(i, slots)
        total = own
        for k in range(slots.shape[0]):
            total = total + slots[k].astype(F32)
        return total

    def spread(peer, share, whole, me):
        i = turn(whole.at[pl.ds(0, OTHERS * rows), :])
        each(OTHERS, lambda k: send(i, share, at_rows(whole, me), peer(k)[1]))
        return i

    def gathered(i):
        await_in(i, owed[i])

    def swap(part, land):
        i = turn(land)
        send(i, part.at[theirs, :], land, across)
        return i

    def z_scatter(part, slots):
        i = turn(slots)

        def one(k):
            _, device, p = z_peer(k)
            send(i, at_rows(part, p), slots.at[k], device)

        each(zs - 1, one)
        return i

    def z_spread(share, whole, me):
        i = turn(whole.at[pl.ds(0, (zs - 1) * rows), :])
        each(zs - 1, lambda k: send(i, share, at_rows(whole, me), z_peer(k)[1]))
        return i

    def forward(whole):
        i = turn(whole.at[pl.ds(0, half), :])
        send(i, whole.at[mine, :], whole.at[mine, :], across)
        return i

    def put(ref, i, value):
        ref[pl.ds(pl.multiple_of(i * rows, rows), rows), :] = value

    def get(ref, i):
        return ref[pl.ds(pl.multiple_of(i * rows, rows), rows), :]

    def direct(cuts, peer, me, total, part, slots, finish, share, whole, beside, behind):
        views = [pl.ds(at, w) for at, w in cuts]
        turns = [scatter(peer, part.at[:, v], b) for v, b in zip(views, slots)]
        beside()
        for n, v in enumerate(views):
            rows_here = pl.ds(pl.multiple_of(me * rows, rows), rows)
            made = finish(v, summed(turns[n], total[rows_here, v], slots[n]))
            share[:, v] = made
            turns[n] = spread(peer, share.at[:, v], whole.at[:, v], me)
            whole[rows_here, v] = made
        behind()
        for i in turns:
            gathered(i)

    def reduced(parts, lands, pairs, slots, finish, shares, wholes, ready=lambda n: None):
        turns = [None] + [swap(parts[1][1], lands[1])]
        turns[0] = scatter(st_peer, parts[0][1], slots[0])
        turns += [swap(p, land) for (_, p), land in zip(parts[2:], lands[2:])]
        last = len(parts) - 1
        for n, (f, _) in list(enumerate(parts))[1:]:
            await_in(turns[n], lands[n])
            pairs[n][...] = (f[mine, :] + lands[n][...].astype(F32)).astype(BF)
            turns[n] = z_scatter(pairs[n], slots[n])
        passed = 0
        for n, (f, _) in enumerate(parts):
            if n == last:
                gathered(turns[0])
                turns[0] = forward(wholes[0])
                passed = 1
            own = get(f, st)
            if n:
                own = own + get(lands[n], z).astype(F32)
            share = finish(n, summed(turns[n], own, slots[n]))
            shares[n][...] = share
            if n < last:
                turns[n] = z_spread(shares[n], wholes[n], st)
            else:
                turns[n] = spread(st_peer, shares[n], wholes[n], st)
            put(wholes[n], st, share)
        for n in range(passed, last):
            gathered(turns[n])
            turns[n] = forward(wholes[n])
        for n, i in enumerate(turns):
            gathered(i)
            ready(n)

    outs = []

    def out(src, dst):
        c = pltpu.make_async_copy(src, dst, out_sem.at[len(outs)])
        c.start()
        outs.append(c)

    for c in loads[:3]:
        c.wait()
    for (f, p), (at, w) in zip(parts1, first):
        cols = pl.ds(at, w)
        part = jnp.concatenate([dot(v_x[...], v_wg[:, cols]), dot(v_x[...], v_wu[:, cols])], axis=1)
        f[...] = part
        p[...] = part.astype(BF)
    for c in loads[3:]:
        c.wait()
    f4[...] = dot(v_th[...], v_td[...])
    pl.semaphore_wait(barrier, 2 * OTHERS)

    def finish_hidden(n, both):
        at, w = first[n]
        gate, up = both[:, :w], both[:, w:]
        gates[:, pl.ds(at, w)] = gate.astype(BF)
        ups[:, pl.ds(at, w)] = up.astype(BF)
        return (gate * jax.nn.sigmoid(gate) * up).astype(BF)

    reduced(parts1, lands1, pairs1, slots1, finish_hidden, shares1, g2)
    part = 0.0
    for g, (at, w) in zip(g2, first):
        part += dot(g[...], v_wd[pl.ds(at, w), :])
    f3[...] = part
    p3[...] = part.astype(BF)
    kept = {}

    def start(name, share, whole):
        put(whole, st, share[...])
        kept[name] = z_spread(share, whole, st)

    def pass_on(name, whole):
        gathered(kept[name])
        kept[name] = forward(whole)

    def beside_down():
        start("gate", gates, gate_ref)
        for g, (at, w) in zip(g2, first):
            out(g, o_hid.at[:, pl.ds(at, w)])

    def finish_features(v, total):
        return (v_stream[:, v].astype(F32) + total).astype(BF)

    direct(
        NARROW, grp_peer, grp, f3, p3, r3, finish_features, g3s, g3,
        beside_down, lambda: start("up", ups, up_ref),
    )
    part = dot(g3[...], v_hd[...]) - f4[...]
    f4[...] = part
    p4[...] = part.astype(BF)

    def finish_signal(v, total):
        return ((total - v_res[:, v].astype(F32)) * (1.0 / math.sqrt(tokens))).astype(BF)

    def beside_error():
        pass_on("gate", gate_ref)
        out(g3, o_feat)

    direct(
        WIDE, st_peer, st, f4, p4, r4, finish_signal, g5s, g5,
        beside_error, lambda: pass_on("up", up_ref),
    )
    part = dot_cols(g5[...], v_hd[...])
    f6[...] = part
    p6[...] = part.astype(BF)
    direct(
        NARROW, grp_peer, grp, f6, p6, r6, lambda v, total: total.astype(BF), g6s, g6,
        lambda: out(g5, o_sig), lambda: None,
    )
    for (f, p), (at, w) in zip(parts7, second):
        part = dot_cols(g6[...], v_wd[pl.ds(at, w), :])
        f[...] = part
        p[...] = part.astype(BF)
    out(g6, o_fg)

    def finish_grad(n, total):
        if n == 0:
            gathered(kept["gate"])
            gathered(kept["up"])
            gate = gate_ref[...].astype(F32)
            sigma = jax.nn.sigmoid(gate)
            by_gate[...] = up_ref[...].astype(F32) * (sigma * (1.0 + gate * (1.0 - sigma)))
            by_up[...] = gate * sigma
        return total.astype(BF)

    def ready_grad(n):
        at, w = second[n]
        cols = pl.ds(at, w)
        grad = g8[n][...].astype(F32)
        for made, by, dest in ((s_gate, by_gate, o_gs), (s_up, by_up, o_us)):
            made[:, cols] = (grad * by[:, cols]).astype(BF)
            out(made.at[:, cols], dest.at[:, cols])

    reduced(parts7, lands7, pairs7, slots7, finish_grad, shares7, g8, ready_grad)
    for i, like in enumerate(owed):
        pltpu.make_async_copy(like, like, send_sem.at[i]).wait()
    for c in outs:
        c.wait()


def gradients(
    x, gs, us, hid, fg, feat, sig, o_gate, o_up, o_down, o_head,
    v_x, v_gs, v_us, v_hid, v_fg, v_feat, v_sig, r_gate, r_up, r_down, r_head,
    load_sem, out_sem,
):
    pairs = [
        (feat, v_feat), (sig, v_sig), (hid, v_hid), (fg, v_fg),
        (x, v_x), (gs, v_gs), (us, v_us),
    ]
    loads = [
        pltpu.make_async_copy(src, dst, load_sem.at[i]) for i, (src, dst) in enumerate(pairs)
    ]
    for c in loads:
        c.start()
    stores = []
    for need, left, right, result, dest in (
        (2, v_feat, v_sig, r_head, o_head),
        (2, v_hid, v_fg, r_down, o_down),
        (2, v_x, v_gs, r_gate, o_gate),
        (1, v_x, v_us, r_up, o_up),
    ):
        for c in loads[:need]:
            c.wait()
        loads = loads[need:]
        result[...] = contract_rows(left[...], right[...])
        c = pltpu.make_async_copy(result, dest, out_sem.at[len(stores)])
        c.start()
        stores.append(c)
    for c in stores:
        c.wait()


def body(
    teacher_hidden, teacher_residual, teacher_down, student_input, student_stream,
    student_gate, student_up, student_down, head,
):
    tokens, ds = student_input.shape
    fs = student_gate.shape[1]
    dt = head.shape[1]
    rows = tokens // N
    arguments = (
        teacher_hidden, teacher_residual, teacher_down, student_input, student_stream,
        student_gate, student_up, student_down, head,
    )
    vm = lambda shape, dtype: pltpu.VMEM(shape, dtype)

    def reduce_bufs(cols):
        return [vm((tokens, cols), F32), vm((tokens, cols), BF)]

    def gather_bufs(cols):
        return [vm((rows, cols), BF), vm((tokens, cols), BF)]

    def block_bufs(cuts, of):
        wide = [w * of for _, w in cuts]
        return (
            [vm((tokens, w), F32) for w in wide]
            + [vm((tokens, w), BF) for w in wide]
            + [vm((tokens // 2, w), BF) for w in wide]
            + [vm((tokens // 2, w), BF) for w in wide]
            + [vm((N // 2 - 1 if n else OTHERS, rows, w), BF) for n, w in enumerate(wide)]
            + [vm((rows, w), BF) for _, w in cuts]
            + [vm((tokens, w), BF) for _, w in cuts]
        )

    staged = [
        vm((rows, a.shape[1]), a.dtype) if i in (1, 4) else vm(a.shape, a.dtype)
        for i, a in enumerate(arguments)
    ]
    scratch = (
        staged
        + reduce_bufs(ds) + gather_bufs(ds)
        + reduce_bufs(dt) + gather_bufs(dt)
        + reduce_bufs(ds) + gather_bufs(ds)
        + gather_bufs(fs) + gather_bufs(fs)
        + [vm((tokens, fs), F32)] * 2
        + [vm((tokens, fs), BF)] * 2
        + [
            pltpu.SemaphoreType.DMA((9,)),
            pltpu.SemaphoreType.DMA((24,)),
            pltpu.SemaphoreType.DMA((64,)),
            pltpu.SemaphoreType.DMA((64,)),
        ]
        + block_bufs(FIRST, 2) + block_bufs(SECOND, 1)
        + [vm((OTHERS, rows, w), BF) for _, w in NARROW + WIDE + NARROW]
    )
    shapes = [(tokens, c) for c in (fs, ds, dt, ds, fs, fs)]
    hidden, features, signal, feature_grad, gate_signal, up_signal = pl.pallas_call(
        functools.partial(kernel, lax.axis_size("tc")),
        out_shape=[jax.ShapeDtypeStruct(s, BF) for s in shapes],
        in_specs=[pl.BlockSpec(memory_space=pl.ANY)] * 9,
        out_specs=[pl.BlockSpec(memory_space=pl.ANY)] * 6,
        scratch_shapes=scratch,
        compiler_params=pltpu.CompilerParams(
            collective_id=0, has_side_effects=True
        ),
        name="chain",
    )(*arguments)
    operands = (student_input, gate_signal, up_signal, hidden, feature_grad, features, signal)
    results = [(ds, fs), (ds, fs), (fs, ds), (ds, dt)]
    return pl.pallas_call(
        gradients,
        out_shape=[jax.ShapeDtypeStruct(s, F32) for s in results],
        in_specs=[pl.BlockSpec(memory_space=pl.ANY)] * 7,
        out_specs=[pl.BlockSpec(memory_space=pl.ANY)] * 4,
        scratch_shapes=[vm(a.shape, a.dtype) for a in operands]
        + [vm(s, F32) for s in results]
        + [pltpu.SemaphoreType.DMA((7,)), pltpu.SemaphoreType.DMA((4,))],
        name="gradients",
    )(*operands)


def solution(mesh):
    in_specs = (
        P(None, "st"),
        P(None, ("tr", "tc")),
        P("st", ("tr", "tc")),
        P(None, "st"),
        P(None, "st"),
        P("st", ("tr", "tc")),
        P("st", ("tr", "tc")),
        P(("tr", "tc"), "st"),
        P("st", ("tr", "tc")),
    )
    out_specs = (
        P("st", ("tr", "tc")),
        P("st", ("tr", "tc")),
        P(("tr", "tc"), "st"),
        P("st", ("tr", "tc")),
    )
    return jax.shard_map(body, mesh=mesh, in_specs=in_specs, out_specs=out_specs, check_vma=False)
```
